32 devices in a mesh: dp: 16 (over z, y, x), mp: 2 (over core).
Axes of the slice: x: 2, y: 2, z: 4, core: 2. Of those that a mesh axis runs over, the one named last changes fastest.
Arguments:
- image_vectors_raw: bfloat16 [6144, 1152], P('dp', 'mp'), may hold values from -0.1796875 to 0.1796875
- text_vectors_raw: bfloat16 [6144, 1152], P('dp', 'mp'), may hold values from -0.1796875 to 0.1796875
- log_logit_scale: float32 [], replicated, may hold values from 0 to 1.5
- bias: float32 [], replicated, may hold values from -3 to -1
- loss_upstream_gradient: float32 [], replicated, may hold values from 0.5 to 2
Outputs:
- image_grad: float32 [6144, 1152], P('dp', 'mp')
- text_grad: float32 [6144, 1152], P('dp', 'mp')
The draws below stay inside these ranges and needn't reach their ends.
All inputs are finite; a program needn't handle non-finite values.
Results may differ from the reference program's by a relative error of at most 0.0039.
Values may be sent and summed in bfloat16 or wider, within the bound.
A program may use at most 64 MiB of HBM per device.

```python
import math
import jax
import jax.numpy as jnp
from jax import lax

E = 1152
ROW_DEV = 384
TURNS = 3
ROWS = 6144


def block_scale(own_key, dims, pieces, least, largest):
    level, own = 1.0, jax.random.fold_in(own_key, 6)
    for position, shards_of in pieces:
        heights = jnp.exp(jax.random.uniform(jax.random.fold_in(own, position), (shards_of,), jnp.float32, least / len(pieces), largest / len(pieces)))
        level = level * jnp.repeat(heights, dims[position] // shards_of).reshape([-1 if axis == position else 1 for axis in range(len(dims))])
    return level


def noise(key, extent, width, bound, split=(), kind=jnp.bfloat16):
    drawn = jax.random.normal(key, extent, jnp.float32) * width
    if len(split) > 0:
        drawn = block_scale(key, extent, split, -0.22, 0.18) * drawn
    return jnp.clip(drawn, min=-bound, max=bound).astype(kind)


def setup_inputs(seed: int = 0) -> dict:
    arg_keys = jax.random.split(jax.random.key(seed), 6)
    return {
        "image_vectors_raw": noise(arg_keys[0], (ROWS, E), 0.03, 0.1796875, ((0, 16), (1, 2))),
        "text_vectors_raw": noise(arg_keys[1], (ROWS, E), 0.03, 0.1796875, ((0, 16), (1, 2))),
        "log_logit_scale": jnp.clip(jax.random.uniform(arg_keys[2], (), jnp.float32, 0.0, 1.5), 0.0, 1.5),
        "bias": jnp.clip(jax.random.uniform(arg_keys[3], (), jnp.float32, -3.0, -1.0), -3.0, -1.0),
        "loss_upstream_gradient": jnp.clip(jnp.exp(jax.random.uniform(arg_keys[4], (), jnp.float32, math.log(0.5), math.log(2.0))), 0.5, 2.0),
    }


def unit_rows(embeds):
    wide = embeds.astype(jnp.float32)
    inverse = lax.rsqrt(lax.optimization_barrier(jnp.sum(wide * wide, axis=1, keepdims=True)) + 1e-06)
    return (wide * inverse, inverse)

def back_norm(unit_wide, inverse, unit_grad):
    inner = lax.optimization_barrier(jnp.sum(unit_wide * unit_grad, axis=1, keepdims=True))
    return inverse * (unit_grad - unit_wide * inner)

def reference(image_vectors_raw, text_vectors_raw, log_logit_scale, bias, loss_upstream_gradient):
    image_wide, inv_image = unit_rows(image_vectors_raw)
    text_wide, inv_text = unit_rows(text_vectors_raw)
    image_unit = image_wide.astype(jnp.bfloat16)
    text_unit = text_wide.astype(jnp.bfloat16)
    logit_scale_value = jnp.exp(log_logit_scale)
    block_rows = ROW_DEV
    block_count = image_vectors_raw.shape[0] // block_rows
    local_ids = jnp.arange(block_rows, dtype=jnp.int32)
    matching_pair = jnp.arange(TURNS * block_rows, dtype=jnp.int32)[None, :] == local_ids[:, None]
    target_signs = jnp.where(matching_pair, 1.0, -1.0).astype(jnp.float32)

    def block_step(block, carry):
        image_acc, text_acc = carry
        partners = (block - jnp.arange(TURNS, dtype=jnp.int32)) % block_count
        rows = (partners[:, None] * block_rows + local_ids[None, :]).reshape(-1).astype(jnp.int32)
        text_block_rows = jnp.take(text_unit, rows, axis=0)
        image_block_rows = lax.dynamic_slice_in_dim(image_unit, (block * block_rows).astype(jnp.int32), block_rows, 0)
        pair_scores = logit_scale_value * jnp.dot(image_block_rows, text_block_rows.T, preferred_element_type=jnp.float32) + bias
        pair_factor = (-loss_upstream_gradient * target_signs * jax.nn.sigmoid(-target_signs * pair_scores) * logit_scale_value).astype(jnp.bfloat16)
        image_part = jnp.dot(pair_factor, text_block_rows, preferred_element_type=jnp.float32)
        image_acc = lax.dynamic_update_slice_in_dim(image_acc, image_part, (block * block_rows).astype(jnp.int32), 0)
        text_acc = text_acc.at[rows].add(jnp.dot(pair_factor.T, image_block_rows, preferred_element_type=jnp.float32))
        return (image_acc, text_acc)
    empty = jnp.zeros(image_wide.shape, jnp.float32)
    image_unit_grad, text_unit_grad = lax.fori_loop(0, block_count, block_step, (empty, empty))
    image_grad = back_norm(image_wide, inv_image, image_unit_grad)
    text_grad = back_norm(text_wide, inv_text, text_unit_grad)
    return (image_grad, text_grad)
```

```python
import functools

import jax
import jax.numpy as jnp
from jax import lax
from jax.experimental import pallas as pl
from jax.experimental.pallas import tpu as pltpu
from jax.sharding import PartitionSpec as P

MESH = pl.DeviceIdType.MESH
F32 = jnp.float32
BF16 = jnp.bfloat16
IMAGE, TEXT = 0, 1
VMEM_LIMIT = 60 << 20


def kernel(
    blocks, parts, chunks,
    image_ref, text_ref, log_scale_ref, bias_ref, upstream_ref,
    image_out, text_out,
    raw, relay, own_unit, own_rows, own_inverse, sums, inner,
    scalars, scalar_sem, load_sem, far_send, far_recv, near_send, near_recv, leg_send, leg_recv,
    own_send, own_recv, share_send, share_recv,
):
    width, rows = image_ref.shape
    size = rows // chunks
    steps = 2 * chunks
    me = lax.axis_index("dp")
    part = lax.axis_index("mp")
    parity = lax.rem(me, 2)
    near = me + 1 - 2 * parity
    late = 1 - parity
    relayed = parity != lax.rem(me // 2, 2)
    direct = jnp.logical_not(relayed)

    def shifted(by):
        return lax.rem(me + blocks + by, blocks)

    def load(ref, side, index):
        return pltpu.make_async_copy(
            ref.at[:, pl.ds(index * size, size)], raw.at[0, side, 0, index], load_sem.at[side, index])

    for index in range(chunks):
        load(image_ref, IMAGE, index).start()
        load(text_ref, TEXT, index).start()
    constants = [
        pltpu.make_async_copy(ref, scalars.at[place], scalar_sem.at[place])
        for place, ref in enumerate((log_scale_ref, bias_ref, upstream_ref))
    ]
    for constant in constants:
        constant.start()

    def side_of(step):
        return jnp.where(step < chunks, parity, 1 - parity)

    def piece(k, side, slot, step):
        return raw.at[k, side, slot, lax.rem(step, chunks)]

    def far_copy(step):
        side = side_of(step)
        return pltpu.make_async_remote_copy(
            src_ref=piece(0, side, 0, step), dst_ref=piece(2, side, 0, step),
            send_sem=far_send.at[step], recv_sem=far_recv.at[step],
            device_id={"dp": shifted(4 * side - 2)}, device_id_type=MESH)

    def leg_copy(index):
        return pltpu.make_async_remote_copy(
            src_ref=raw.at[0, late, 0, index], dst_ref=relay.at[index],
            send_sem=leg_send.at[index], recv_sem=leg_recv.at[index],
            device_id={"dp": shifted(8 * late - 4)}, device_id_type=MESH)

    def relay_copy(index):
        return pltpu.make_async_remote_copy(
            src_ref=relay.at[index], dst_ref=raw.at[2, late, 0, index],
            send_sem=far_send.at[chunks + index], recv_sem=far_recv.at[chunks + index],
            device_id={"dp": shifted(2 - 4 * late)}, device_id_type=MESH)

    def near_copy(step, k):
        side = 1 - side_of(step)
        return pltpu.make_async_remote_copy(
            src_ref=piece(k, side, 0, step), dst_ref=piece(1, side, 0, step),
            send_sem=near_send.at[step], recv_sem=near_recv.at[step],
            device_id={"dp": near}, device_id_type=MESH)

    def own_copy(side, offset):
        return pltpu.make_async_remote_copy(
            src_ref=raw.at[0, side, 0], dst_ref=raw.at[0, side, parts - offset],
            send_sem=own_send.at[side, offset], recv_sem=own_recv.at[side, parts - offset],
            device_id={"mp": lax.rem(part + offset, parts)}, device_id_type=MESH)

    def share_copy(k, step, offset):
        side = side_of(step)
        return pltpu.make_async_remote_copy(
            src_ref=piece(k, side, 0, step), dst_ref=piece(k, side, parts - offset, step),
            send_sem=share_send.at[k - 1, step, offset], recv_sem=share_recv.at[k - 1, step, parts - offset],
            device_id={"mp": lax.rem(part + offset, parts)}, device_id_type=MESH)

    barrier = pltpu.get_barrier_semaphore()

    def greet(target):
        pl.semaphore_signal(barrier, inc=1, device_id={"dp": target}, device_id_type=MESH)

    @pl.when(relayed)
    def _():
        greet(shifted(2))
        greet(shifted(-2))
        greet(shifted(4 - 8 * late))

    @pl.when(direct)
    def _():
        greet(shifted(2 - 4 * parity))

    greet(near)
    for offset in range(1, parts):
        pl.semaphore_signal(barrier, inc=1, device_id={"mp": lax.rem(part + offset, parts)}, device_id_type=MESH)
    pl.semaphore_wait(barrier, 2 + parts)

    for step in range(chunks):
        load(image_ref, IMAGE, step).wait()
        load(text_ref, TEXT, step).wait()
        far_copy(step).start()
        near_copy(step, 0).start()

    @pl.when(relayed)
    def _():
        for index in range(chunks):
            leg_copy(index).start()

    @pl.when(direct)
    def _():
        for step in range(chunks, steps):
            far_copy(step).start()

    for side in (IMAGE, TEXT):
        for offset in range(1, parts):
            own_copy(side, offset).start()

    for constant in constants:
        constant.wait()
    scale = jnp.exp(jnp.zeros((1, 1), F32) + scalars[0, 0])
    bias = scalars[1, 0]
    weight = scale * scalars[2, 0]

    def unit_rows(k, side, index):
        wide = [raw[k, side, slot, index].astype(F32) for slot in range(parts)]
        square = sum(jnp.sum(w * w, axis=0, keepdims=True) for w in wide)
        inverse = lax.rsqrt(square + 1e-06)
        return [(w * inverse).astype(BF16) for w in wide], inverse

    def pair_terms(units, side, diagonal):
        other = 1 - side
        total = None
        for slot in range(parts):
            term = jnp.dot(own_rows[other, slot], units[slot], preferred_element_type=F32)
            total = term if total is None else total + term
        scores = scale * total + bias
        if diagonal:
            shape = total.shape
            matching = lax.broadcasted_iota(jnp.int32, shape, 0) == lax.broadcasted_iota(jnp.int32, shape, 1)
            sign = jnp.where(matching, 1.0, -1.0).astype(F32)
            factor = -weight * sign * jax.nn.sigmoid(-sign * scores)
        else:
            factor = weight * jax.nn.sigmoid(scores)
        factor = factor.astype(BF16)
        gradient = lax.dot_general(
            units[0], factor, (((1,), (1,)), ((), ())), preferred_element_type=F32)
        product = factor.astype(F32) * total
        product = sum(product[:, at:at + size] for at in range(0, product.shape[1], size))
        if diagonal:
            sums[other] = gradient
            inner[other] = product
        else:
            sums[other] += gradient
            inner[other] += product

    for side in (IMAGE, TEXT):
        for slot in range(1, parts):
            own_copy(side, parts - slot).wait_recv()

    def own_norm(index, carry):
        side, place = index // chunks, lax.rem(index, chunks)
        units, inverse = unit_rows(0, side, place)
        for slot in range(parts):
            own_unit[side, slot, place] = units[slot]
            own_rows[side, slot, pl.ds(pl.multiple_of(place * size, size), size), :] = units[slot].T
        own_inverse[side, place] = inverse
        return carry

    lax.fori_loop(0, steps, own_norm, 0)

    def own_pairs(side, carry):
        pair_terms(
            [jnp.concatenate([own_unit[side, slot, place] for place in range(chunks)], axis=1)
             for slot in range(parts)], side, True)
        return carry

    lax.fori_loop(0, 2, own_pairs, 0)

    def finish(side, out):
        for index in range(chunks):
            place = slice(index * size, (index + 1) * size)
            inverse = own_inverse[side, index]
            product = jnp.sum(inner[side, place, :].T, axis=0, keepdims=True)
            unit = raw[0, side, 0, index].astype(F32) * inverse
            out[:, place] = inverse * (sums[side, :, place] - unit * product)

    def advance(step, carry):
        @pl.when(step < steps)
        def _():
            far_copy(step).wait_recv()

            @pl.when(step < chunks)
            def _():
                near_copy(step + chunks, 2).start()

            @pl.when((step < chunks) & relayed)
            def _():
                leg_copy(step).wait_recv()
                relay_copy(step).start()

            for offset in range(1, parts):
                share_copy(2, step, offset).start()
            near_copy(step, 0).wait_recv()
            for offset in range(1, parts):
                share_copy(1, step, offset).start()

        @pl.when(step > 0)
        def _():
            past = step - 1
            side = side_of(past)
            for k in (1, 2):
                for slot in range(1, parts):
                    share_copy(k, past, parts - slot).wait_recv()
            units = [unit_rows(k, side, lax.rem(past, chunks))[0] for k in (1, 2)]
            pair_terms([jnp.concatenate(halves, axis=1) for halves in zip(*units)], side, False)

        @pl.when((step == chunks) & (parity == 0))
        def _():
            finish(TEXT, text_out)

        @pl.when((step == chunks) & (parity == 1))
        def _():
            finish(IMAGE, image_out)

        return carry

    lax.fori_loop(0, steps + 1, advance, 0)

    @pl.when(parity == 0)
    def _():
        finish(IMAGE, image_out)

    @pl.when(parity == 1)
    def _():
        finish(TEXT, text_out)

    for side in (IMAGE, TEXT):
        for offset in range(1, parts):
            own_copy(side, offset).wait_send()

    @pl.when(relayed)
    def _():
        for index in range(chunks):
            leg_copy(index).wait_send()
            relay_copy(index).wait_send()

    @pl.when(direct)
    def _():
        for step in range(chunks, steps):
            far_copy(step).wait_send()

    for step in range(steps):
        if step < chunks:
            far_copy(step).wait_send()
        near_copy(step, 0).wait_send()
        for offset in range(1, parts):
            share_copy(1, step, offset).wait_send()
            share_copy(2, step, offset).wait_send()


def publish(image_ref, text_ref, image_out, text_out, sems):
    copies = [
        pltpu.make_async_copy(image_ref, image_out, sems.at[0]),
        pltpu.make_async_copy(text_ref, text_out, sems.at[1]),
    ]
    for copy in copies:
        copy.start()
    for copy in copies:
        copy.wait()


def solution(mesh):
    blocks, parts = mesh.shape["dp"], mesh.shape["mp"]

    def local(image, text, log_logit_scale, bias, loss_upstream_gradient):
        rows, width = image.shape
        chunks = max(rows // 128, 1)
        size = rows // chunks
        steps = 2 * chunks
        hbm = pl.BlockSpec(memory_space=pltpu.HBM)
        anywhere = pl.BlockSpec(memory_space=pl.ANY)
        whole = pl.BlockSpec(memory_space=pltpu.VMEM)
        dma = pltpu.SemaphoreType.DMA
        out = jax.ShapeDtypeStruct((width, rows), F32)
        image_grad, text_grad = pl.pallas_call(
            functools.partial(kernel, blocks, parts, chunks),
            out_shape=(pltpu.VMEM((width, rows), F32),) * 2,
            in_specs=[hbm] * 5,
            out_specs=(whole, whole),
            scratch_shapes=[
                pltpu.VMEM((3, 2, parts, chunks, width, size), BF16),
                pltpu.VMEM((chunks, width, size), BF16),
                pltpu.VMEM((2, parts, chunks, width, size), BF16),
                pltpu.VMEM((2, parts, rows, width), BF16),
                pltpu.VMEM((2, chunks, 1, size), F32),
                pltpu.VMEM((2, width, rows), F32),
                pltpu.VMEM((2, rows, size), F32),
                pltpu.SMEM((3, 1), F32), dma((3,)), dma((2, chunks)),
                dma((steps,)), dma((steps,)), dma((steps,)), dma((steps,)),
                dma((chunks,)), dma((chunks,)),
                dma((2, parts)), dma((2, parts)),
                dma((2, steps, parts)), dma((2, steps, parts)),
            ],
            compiler_params=pltpu.CompilerParams(
                collective_id=0, has_side_effects=True, vmem_limit_bytes=VMEM_LIMIT),
        )(image.T, text.T, log_logit_scale.reshape(1), bias.reshape(1), loss_upstream_gradient.reshape(1))
        image_grad, text_grad = pl.pallas_call(
            publish,
            out_shape=(out, out),
            in_specs=[anywhere, anywhere],
            out_specs=(hbm, hbm),
            scratch_shapes=[dma((2,))],
            compiler_params=pltpu.CompilerParams(vmem_limit_bytes=4 << 20),
        )(image_grad, text_grad)
        return image_grad.T, text_grad.T

    placed = (P("dp", "mp"), P("dp", "mp"), P(), P(), P())
    return jax.shard_map(
        local, mesh=mesh, in_specs=placed, out_specs=(P("dp", "mp"), P("dp", "mp")), check_vma=False
    )
```

```python
import functools

import jax
import jax.numpy as jnp
from jax import lax
from jax.experimental import pallas as pl
from jax.experimental.pallas import tpu as pltpu
from jax.sharding import PartitionSpec as P

MESH = pl.DeviceIdType.MESH
F32 = jnp.float32
BF16 = jnp.bfloat16
IMAGE, TEXT = 0, 1
VMEM_LIMIT = 60 << 20


def kernel(
    blocks, parts, chunks,
    image_ref, text_ref, constant_ref,
    image_out, text_out,
    raw, relay, own_unit, own_rows, own_inverse, sums, inner, constants,
    load_sem, constant_send, constant_recv, far_send, far_recv, near_send, near_recv, leg_send, leg_recv,
    own_send, own_recv, share_send, share_recv,
):
    width, rows = image_ref.shape
    size = rows // chunks
    steps = 2 * chunks
    me = lax.axis_index("dp")
    part = lax.axis_index("mp")
    parity = lax.rem(me, 2)
    near = me + 1 - 2 * parity
    late = 1 - parity
    relayed = parity != lax.rem(me // 2, 2)
    direct = jnp.logical_not(relayed)
    members = 2 * parts
    member = parity * parts + part

    def shifted(by):
        return lax.rem(me + blocks + by, blocks)

    def load(ref, side, index):
        return pltpu.make_async_copy(
            ref.at[:, pl.ds(index * size, size)], raw.at[0, side, 0, index], load_sem)

    for index in range(chunks):
        load(image_ref, IMAGE, index).start()
        load(text_ref, TEXT, index).start()
    constants[member] = constant_ref[...]

    def settle(ref, sem):
        pltpu.make_async_copy(ref, ref, sem).wait()

    def mate(offset):
        other = lax.rem(member + offset, members)
        return {"dp": me - parity + other // parts, "mp": lax.rem(other, parts)}

    def constant_copy(offset):
        return pltpu.make_async_remote_copy(
            src_ref=constant_ref, dst_ref=constants.at[member],
            send_sem=constant_send, recv_sem=constant_recv,
            device_id=mate(offset), device_id_type=MESH)

    def side_of(step):
        return jnp.where(step < chunks, parity, 1 - parity)

    def piece(k, side, slot, step):
        return raw.at[k, side, slot, lax.rem(step, chunks)]

    def far_copy(step):
        side = side_of(step)
        return pltpu.make_async_remote_copy(
            src_ref=piece(0, side, 0, step), dst_ref=piece(2, side, 0, step),
            send_sem=far_send, recv_sem=far_recv.at[step],
            device_id={"dp": shifted(4 * side - 2)}, device_id_type=MESH)

    def leg_copy(index):
        return pltpu.make_async_remote_copy(
            src_ref=raw.at[0, late, 0, index], dst_ref=relay.at[index],
            send_sem=leg_send, recv_sem=leg_recv.at[index],
            device_id={"dp": shifted(8 * late - 4)}, device_id_type=MESH)

    def relay_copy(index):
        return pltpu.make_async_remote_copy(
            src_ref=relay.at[index], dst_ref=raw.at[2, late, 0, index],
            send_sem=far_send, recv_sem=far_recv.at[chunks + index],
            device_id={"dp": shifted(2 - 4 * late)}, device_id_type=MESH)

    def near_copy(step, k):
        side = 1 - side_of(step)
        return pltpu.make_async_remote_copy(
            src_ref=piece(k, side, 0, step), dst_ref=piece(1, side, 0, step),
            send_sem=near_send, recv_sem=near_recv.at[step],
            device_id={"dp": near}, device_id_type=MESH)

    def own_copy(side, offset):
        return pltpu.make_async_remote_copy(
            src_ref=raw.at[0, side, 0], dst_ref=raw.at[0, side, parts - offset],
            send_sem=own_send.at[offset - 1], recv_sem=own_recv.at[parts - offset - 1],
            device_id={"mp": lax.rem(part + offset, parts)}, device_id_type=MESH)

    def share_copy(k, step, offset):
        side = side_of(step)
        return pltpu.make_async_remote_copy(
            src_ref=piece(k, side, 0, step), dst_ref=piece(k, side, parts - offset, step),
            send_sem=share_send.at[offset - 1], recv_sem=share_recv.at[step, parts - offset - 1],
            device_id={"mp": lax.rem(part + offset, parts)}, device_id_type=MESH)

    barrier = pltpu.get_barrier_semaphore()

    def greet(target):
        pl.semaphore_signal(barrier, inc=1, device_id={"dp": target}, device_id_type=MESH)

    @pl.when(relayed)
    def _():
        greet(shifted(2))
        greet(shifted(-2))
        greet(shifted(4 - 8 * late))

    @pl.when(direct)
    def _():
        greet(shifted(2 - 4 * parity))

    for offset in range(1, members):
        pl.semaphore_signal(barrier, inc=1, device_id=mate(offset), device_id_type=MESH)
    settle(raw.at[0, :, 0], load_sem)
    pl.semaphore_wait(barrier, 1 + members)

    for offset in range(1, members):
        constant_copy(offset).start()
    for step in range(chunks):
        far_copy(step).start()
        near_copy(step, 0).start()

    @pl.when(relayed)
    def _():
        for index in range(chunks):
            leg_copy(index).start()

    @pl.when(direct)
    def _():
        for step in range(chunks, steps):
            far_copy(step).start()

    for side in (IMAGE, TEXT):
        for offset in range(1, parts):
            own_copy(side, offset).start()

    def unit_rows(k, side, index):
        wide = [raw[k, side, slot, index].astype(F32) for slot in range(parts)]
        square = sum(jnp.sum(w * w, axis=0, keepdims=True) for w in wide)
        inverse = lax.rsqrt(square + 1e-06)
        return [(w * inverse).astype(BF16) for w in wide], inverse

    def pair_terms(units, side, diagonal):
        other = 1 - side
        scale = jnp.exp(constants[0, :, 0:1])
        bias = constants[1, :, 0:1]
        weight = scale * constants[2, :, 0:1]
        total = None
        for slot in range(parts):
            term = jnp.dot(own_rows[other, slot], units[slot], preferred_element_type=F32)
            total = term if total is None else total + term
        scores = scale * total + bias
        if diagonal:
            shape = total.shape
            matching = lax.broadcasted_iota(jnp.int32, shape, 0) == lax.broadcasted_iota(jnp.int32, shape, 1)
            sign = jnp.where(matching, 1.0, -1.0).astype(F32)
            factor = -weight * sign * jax.nn.sigmoid(-sign * scores)
        else:
            factor = weight * jax.nn.sigmoid(scores)
        factor = factor.astype(BF16)
        gradient = lax.dot_general(
            units[0], factor, (((1,), (1,)), ((), ())), preferred_element_type=F32)
        product = factor.astype(F32) * total
        product = sum(product[:, at:at + size] for at in range(0, product.shape[1], size))
        if diagonal:
            sums[other] = gradient
            inner[other] = product
        else:
            sums[other] += gradient
            inner[other] += product

    for slot in range(1, parts):
        settle(raw.at[0, :, slot], own_recv.at[slot - 1])

    def own_norm(index, carry):
        side, place = index // chunks, lax.rem(index, chunks)
        units, inverse = unit_rows(0, side, place)
        for slot in range(parts):
            own_unit[side, slot, place] = units[slot]
            own_rows[side, slot, pl.ds(pl.multiple_of(place * size, size), size), :] = units[slot].T
        own_inverse[side, place] = inverse
        return carry

    lax.fori_loop(0, steps, own_norm, 0)
    settle(constants.at[pl.ds(1, members - 1)], constant_recv)

    def own_pairs(side, carry):
        pair_terms(
            [jnp.concatenate([own_unit[side, slot, place] for place in range(chunks)], axis=1)
             for slot in range(parts)], side, True)
        return carry

    lax.fori_loop(0, 2, own_pairs, 0)

    def finish(side, out):
        for index in range(chunks):
            place = slice(index * size, (index + 1) * size)
            inverse = own_inverse[side, index]
            product = jnp.sum(inner[side, place, :].T, axis=0, keepdims=True)
            unit = raw[0, side, 0, index].astype(F32) * inverse
            out[:, place] = inverse * (sums[side, :, place] - unit * product)

    def advance(step, carry):
        @pl.when(step < steps)
        def _():
            far_copy(step).wait_recv()

            @pl.when(step < chunks)
            def _():
                near_copy(step + chunks, 2).start()

            @pl.when((step < chunks) & relayed)
            def _():
                leg_copy(step).wait_recv()
                relay_copy(step).start()

            for offset in range(1, parts):
                share_copy(2, step, offset).start()
            near_copy(step, 0).wait_recv()
            for offset in range(1, parts):
                share_copy(1, step, offset).start()

        @pl.when(step > 0)
        def _():
            past = step - 1
            side = side_of(past)
            for slot in range(1, parts):
                settle(raw.at[pl.ds(1, 2), side, slot, lax.rem(past, chunks)], share_recv.at[past, slot - 1])
            units = [unit_rows(k, side, lax.rem(past, chunks))[0] for k in (1, 2)]
            pair_terms([jnp.concatenate(halves, axis=1) for halves in zip(*units)], side, False)

        @pl.when((step == chunks) & (parity == 0))
        def _():
            finish(TEXT, text_out)

        @pl.when((step == chunks) & (parity == 1))
        def _():
            finish(IMAGE, image_out)

        return carry

    lax.fori_loop(0, steps + 1, advance, 0)

    @pl.when(parity == 0)
    def _():
        finish(IMAGE, image_out)

    @pl.when(parity == 1)
    def _():
        finish(TEXT, text_out)

    @pl.when(relayed)
    def _():
        settle(relay, leg_send)

    settle(raw.at[0, :, 0], far_send)
    settle(raw.at[0, :, 0], near_send)
    settle(constants.at[pl.ds(1, members - 1)], constant_send)
    for offset in range(1, parts):
        settle(raw.at[0, :, 0], own_send.at[offset - 1])
        settle(raw.at[pl.ds(0, 2), :, 0], share_send.at[offset - 1])


def spread(value_ref, row_ref):
    row_ref[...] = jnp.full(row_ref.shape, value_ref[0])


def publish(image_ref, text_ref, image_out, text_out, sems):
    copies = [
        pltpu.make_async_copy(image_ref, image_out, sems.at[0]),
        pltpu.make_async_copy(text_ref, text_out, sems.at[1]),
    ]
    for copy in copies:
        copy.start()
    for copy in copies:
        copy.wait()


def solution(mesh):
    blocks, parts = mesh.shape["dp"], mesh.shape["mp"]

    def local(image, text, log_logit_scale, bias, loss_upstream_gradient):
        rows, width = image.shape
        chunks = max(rows // 128, 1)
        size = rows // chunks
        steps = 2 * chunks
        hbm = pl.BlockSpec(memory_space=pltpu.HBM)
        anywhere = pl.BlockSpec(memory_space=pl.ANY)
        whole = pl.BlockSpec(memory_space=pltpu.VMEM)
        dma = pltpu.SemaphoreType.DMA
        out = jax.ShapeDtypeStruct((width, rows), F32)
        member = lax.rem(lax.axis_index("dp"), 2) * parts + lax.axis_index("mp")

        def pick(place):
            def branch(*values):
                return pl.pallas_call(
                    spread,
                    out_shape=pltpu.VMEM((1, 128), F32),
                    in_specs=[pl.BlockSpec(memory_space=pltpu.SMEM)],
                    out_specs=whole,
                    name=f"constant_{place}",
                    compiler_params=pltpu.CompilerParams(vmem_limit_bytes=1 << 20),
                )(values[place].reshape(1))
            return branch

        constant = lax.switch(
            lax.rem(member, 3), [pick(place) for place in range(3)], log_logit_scale, bias, loss_upstream_gradient)
        image_grad, text_grad = pl.pallas_call(
            functools.partial(kernel, blocks, parts, chunks),
            out_shape=(pltpu.VMEM((width, rows), F32),) * 2,
            in_specs=[hbm, hbm, whole],
            out_specs=(whole, whole),
            scratch_shapes=[
                pltpu.VMEM((3, 2, parts, chunks, width, size), BF16),
                pltpu.VMEM((chunks, width, size), BF16),
                pltpu.VMEM((2, parts, chunks, width, size), BF16),
                pltpu.VMEM((2, parts, rows, width), BF16),
                pltpu.VMEM((2, chunks, 1, size), F32),
                pltpu.VMEM((2, width, rows), F32),
                pltpu.VMEM((2, rows, size), F32),
                pltpu.VMEM((2 * parts, 1, 128), F32),
                dma, dma, dma, dma, dma((steps,)), dma, dma((steps,)), dma, dma((chunks,)),
                dma((parts - 1,)), dma((parts - 1,)),
                dma((parts - 1,)), dma((steps, parts - 1)),
            ],
            compiler_params=pltpu.CompilerParams(
                collective_id=0, has_side_effects=True, vmem_limit_bytes=VMEM_LIMIT),
        )(image.T, text.T, constant)
        image_grad, text_grad = pl.pallas_call(
            publish,
            out_shape=(out, out),
            in_specs=[anywhere, anywhere],
            out_specs=(hbm, hbm),
            scratch_shapes=[dma((2,))],
            compiler_params=pltpu.CompilerParams(vmem_limit_bytes=4 << 20),
        )(image_grad, text_grad)
        return image_grad.T, text_grad.T

    placed = (P("dp", "mp"), P("dp", "mp"), P(), P(), P())
    return jax.shard_map(
        local, mesh=mesh, in_specs=placed, out_specs=(P("dp", "mp"), P("dp", "mp")), check_vma=False
    )
```

```python
import functools

import jax
import jax.numpy as jnp
from jax import lax
from jax.experimental import pallas as pl
from jax.experimental.pallas import tpu as pltpu
from jax.sharding import PartitionSpec as P

MESH = pl.DeviceIdType.MESH
F32 = jnp.float32
BF16 = jnp.bfloat16
IMAGE, TEXT = 0, 1
VMEM_LIMIT = 60 << 20


def kernel(
    blocks, parts, chunks,
    image_ref, text_ref, constant_ref,
    image_out, text_out,
    raw, relay, own_unit, own_rows, own_inverse, sums, inner, constants,
    load_sem, constant_send, constant_recv, far_send, far_recv, near_send, near_recv, leg_send, leg_recv,
    own_send, own_recv, share_send, share_recv, token,
):
    width, rows = image_ref.shape
    size = rows // chunks
    steps = 2 * chunks
    me = lax.axis_index("dp")
    part = lax.axis_index("mp")
    parity = lax.rem(me, 2)
    near = me + 1 - 2 * parity
    late = 1 - parity
    row = lax.rem(me // 2, 2)
    relayed = parity != row
    direct = jnp.logical_not(relayed)
    members = 2 * parts
    member = parity * parts + part

    def shifted(by):
        return lax.rem(me + blocks + by, blocks)

    def load(ref, side, index):
        return pltpu.make_async_copy(
            ref.at[:, pl.ds(index * size, size)], raw.at[0, side, 0, index], load_sem)

    for index in range(chunks):
        load(image_ref, IMAGE, index).start()
        load(text_ref, TEXT, index).start()
    constants[member] = constant_ref[...]

    def settle(ref, sem):
        pltpu.make_async_copy(ref, ref, sem).wait()

    def mate(offset):
        other = lax.rem(member + offset, members)
        return {"dp": me - parity + other // parts, "mp": lax.rem(other, parts)}

    def constant_copy(offset):
        return pltpu.make_async_remote_copy(
            src_ref=constant_ref, dst_ref=constants.at[member],
            send_sem=constant_send, recv_sem=constant_recv,
            device_id=mate(offset), device_id_type=MESH)

    def side_of(step):
        return jnp.where(step < chunks, parity, 1 - parity)

    def piece(k, side, slot, step):
        return raw.at[k, side, slot, lax.rem(step, chunks)]

    def far_copy(step):
        side = side_of(step)
        return pltpu.make_async_remote_copy(
            src_ref=piece(0, side, 0, step), dst_ref=piece(2, side, 0, step),
            send_sem=far_send, recv_sem=far_recv.at[step],
            device_id={"dp": shifted(4 * side - 2)}, device_id_type=MESH)

    def leg_copy(index):
        return pltpu.make_async_remote_copy(
            src_ref=raw.at[0, late, 0, index], dst_ref=relay.at[index],
            send_sem=leg_send, recv_sem=leg_recv.at[index],
            device_id={"dp": shifted(8 * late - 4)}, device_id_type=MESH)

    def relay_copy(index):
        return pltpu.make_async_remote_copy(
            src_ref=relay.at[index], dst_ref=raw.at[2, late, 0, index],
            send_sem=far_send, recv_sem=far_recv.at[chunks + index],
            device_id={"dp": shifted(2 - 4 * late)}, device_id_type=MESH)

    def near_copy(step, k):
        side = 1 - side_of(step)
        return pltpu.make_async_remote_copy(
            src_ref=piece(k, side, 0, step), dst_ref=piece(1, side, 0, step),
            send_sem=near_send, recv_sem=near_recv.at[step],
            device_id={"dp": near}, device_id_type=MESH)

    def own_copy(side, offset):
        return pltpu.make_async_remote_copy(
            src_ref=raw.at[0, side, 0], dst_ref=raw.at[0, side, parts - offset],
            send_sem=own_send.at[offset - 1], recv_sem=own_recv.at[parts - offset - 1],
            device_id={"mp": lax.rem(part + offset, parts)}, device_id_type=MESH)

    def share_copy(k, step, offset):
        side = side_of(step)
        return pltpu.make_async_remote_copy(
            src_ref=piece(k, side, 0, step), dst_ref=piece(k, side, parts - offset, step),
            send_sem=share_send.at[offset - 1], recv_sem=share_recv.at[step, parts - offset - 1],
            device_id={"mp": lax.rem(part + offset, parts)}, device_id_type=MESH)

    barrier = pltpu.get_barrier_semaphore()

    def greet(target):
        pl.semaphore_signal(barrier, inc=1, device_id={"dp": target}, device_id_type=MESH)

    greet(shifted(2 - 4 * row))

    @pl.when(relayed)
    def _():
        greet(shifted(-2 - 2 * row))

    for offset in range(1, members):
        pl.semaphore_signal(barrier, inc=1, device_id=mate(offset), device_id_type=MESH)
    settle(raw.at[0, :, 0], load_sem)
    pl.semaphore_wait(barrier, row + members)

    for offset in range(1, members):
        constant_copy(offset).start()

    def inform(target):
        pl.semaphore_signal(token, inc=1, device_id={"dp": target}, device_id_type=MESH)

    @pl.when(row == 1)
    def _():
        inform(shifted(4 - 2 * parity))

    for step in range(chunks):
        @pl.when(parity + row > 0)
        def _():
            far_copy(step).start()

        near_copy(step, 0).start()

    @pl.when(direct)
    def _():
        for step in range(chunks, steps):
            far_copy(step).start()

    for side in (IMAGE, TEXT):
        for offset in range(1, parts):
            own_copy(side, offset).start()

    def unit_rows(k, side, index):
        wide = [raw[k, side, slot, index].astype(F32) for slot in range(parts)]
        square = sum(jnp.sum(w * w, axis=0, keepdims=True) for w in wide)
        inverse = lax.rsqrt(square + 1e-06)
        return [(w * inverse).astype(BF16) for w in wide], inverse

    def pair_terms(units, side, diagonal):
        other = 1 - side
        scale = jnp.exp(constants[0, :, 0:1])
        bias = constants[1, :, 0:1]
        weight = scale * constants[2, :, 0:1]
        total = None
        for slot in range(parts):
            term = jnp.dot(own_rows[other, slot], units[slot], preferred_element_type=F32)
            total = term if total is None else total + term
        scores = scale * total + bias
        if diagonal:
            shape = total.shape
            matching = lax.broadcasted_iota(jnp.int32, shape, 0) == lax.broadcasted_iota(jnp.int32, shape, 1)
            sign = jnp.where(matching, 1.0, -1.0).astype(F32)
            factor = -weight * sign * jax.nn.sigmoid(-sign * scores)
        else:
            factor = weight * jax.nn.sigmoid(scores)
        factor = factor.astype(BF16)
        gradient = lax.dot_general(
            units[0], factor, (((1,), (1,)), ((), ())), preferred_element_type=F32)
        product = factor.astype(F32) * total
        product = sum(product[:, at:at + size] for at in range(0, product.shape[1], size))
        if diagonal:
            sums[other] = gradient
            inner[other] = product
        else:
            sums[other] += gradient
            inner[other] += product

    @pl.when((parity == 0) & (row == 1))
    def _():
        for index in range(chunks):
            leg_copy(index).start()
        pl.semaphore_wait(token, 1)
        inform(shifted(-2))

    @pl.when((parity == 0) & (row == 0))
    def _():
        pl.semaphore_wait(token, 1)
        for step in range(chunks):
            far_copy(step).start()

    @pl.when((parity == 1) & (row == 0))
    def _():
        pl.semaphore_wait(token, 1)
        for index in range(chunks):
            leg_copy(index).start()

    for slot in range(1, parts):
        settle(raw.at[0, :, slot], own_recv.at[slot - 1])

    def own_norm(index, carry):
        side, place = index // chunks, lax.rem(index, chunks)
        units, inverse = unit_rows(0, side, place)
        for slot in range(parts):
            own_unit[side, slot, place] = units[slot]
            own_rows[side, slot, pl.ds(pl.multiple_of(place * size, size), size), :] = units[slot].T
        own_inverse[side, place] = inverse
        return carry

    lax.fori_loop(0, steps, own_norm, 0)
    settle(constants.at[pl.ds(1, members - 1)], constant_recv)

    def own_pairs(side, carry):
        pair_terms(
            [jnp.concatenate([own_unit[side, slot, place] for place in range(chunks)], axis=1)
             for slot in range(parts)], side, True)
        return carry

    lax.fori_loop(0, 2, own_pairs, 0)

    def finish(side, out):
        for index in range(chunks):
            place = slice(index * size, (index + 1) * size)
            inverse = own_inverse[side, index]
            product = jnp.sum(inner[side, place, :].T, axis=0, keepdims=True)
            unit = raw[0, side, 0, index].astype(F32) * inverse
            out[:, place] = inverse * (sums[side, :, place] - unit * product)

    def advance(step, carry):
        @pl.when(step < steps)
        def _():
            far_copy(step).wait_recv()

            @pl.when(step < chunks)
            def _():
                near_copy(step + chunks, 2).start()

            @pl.when((step < chunks) & relayed)
            def _():
                leg_copy(step).wait_recv()
                relay_copy(step).start()

            for offset in range(1, parts):
                share_copy(2, step, offset).start()
            near_copy(step, 0).wait_recv()
            for offset in range(1, parts):
                share_copy(1, step, offset).start()

        @pl.when(step > 0)
        def _():
            past = step - 1
            side = side_of(past)
            for slot in range(1, parts):
                settle(raw.at[pl.ds(1, 2), side, slot, lax.rem(past, chunks)], share_recv.at[past, slot - 1])
            units = [unit_rows(k, side, lax.rem(past, chunks))[0] for k in (1, 2)]
            pair_terms([jnp.concatenate(halves, axis=1) for halves in zip(*units)], side, False)

        @pl.when((step == chunks) & (parity == 0))
        def _():
            finish(TEXT, text_out)

        @pl.when((step == chunks) & (parity == 1))
        def _():
            finish(IMAGE, image_out)

        return carry

    lax.fori_loop(0, steps + 1, advance, 0)

    @pl.when(parity == 0)
    def _():
        finish(IMAGE, image_out)

    @pl.when(parity == 1)
    def _():
        finish(TEXT, text_out)

    @pl.when(relayed)
    def _():
        settle(relay, leg_send)

    settle(raw.at[0, :, 0], far_send)
    settle(raw.at[0, :, 0], near_send)
    settle(constants.at[pl.ds(1, members - 1)], constant_send)
    for offset in range(1, parts):
        settle(raw.at[0, :, 0], own_send.at[offset - 1])
        settle(raw.at[pl.ds(0, 2), :, 0], share_send.at[offset - 1])


def spread(value_ref, row_ref):
    row_ref[...] = jnp.full(row_ref.shape, value_ref[0])


def publish(image_ref, text_ref, image_out, text_out, sems):
    copies = [
        pltpu.make_async_copy(image_ref, image_out, sems.at[0]),
        pltpu.make_async_copy(text_ref, text_out, sems.at[1]),
    ]
    for copy in copies:
        copy.start()
    for copy in copies:
        copy.wait()


def solution(mesh):
    blocks, parts = mesh.shape["dp"], mesh.shape["mp"]

    def local(image, text, log_logit_scale, bias, loss_upstream_gradient):
        rows, width = image.shape
        chunks = max(rows // 128, 1)
        size = rows // chunks
        steps = 2 * chunks
        hbm = pl.BlockSpec(memory_space=pltpu.HBM)
        anywhere = pl.BlockSpec(memory_space=pl.ANY)
        whole = pl.BlockSpec(memory_space=pltpu.VMEM)
        dma = pltpu.SemaphoreType.DMA
        out = jax.ShapeDtypeStruct((width, rows), F32)
        member = lax.rem(lax.axis_index("dp"), 2) * parts + lax.axis_index("mp")

        def pick(place):
            def branch(*values):
                return pl.pallas_call(
                    spread,
                    out_shape=pltpu.VMEM((1, 128), F32),
                    in_specs=[pl.BlockSpec(memory_space=pltpu.SMEM)],
                    out_specs=whole,
                    name=f"constant_{place}",
                    compiler_params=pltpu.CompilerParams(vmem_limit_bytes=1 << 20),
                )(values[place].reshape(1))
            return branch

        constant = lax.switch(
            lax.rem(member, 3), [pick(place) for place in range(3)], log_logit_scale, bias, loss_upstream_gradient)
        image_grad, text_grad = pl.pallas_call(
            functools.partial(kernel, blocks, parts, chunks),
            out_shape=(pltpu.VMEM((width, rows), F32),) * 2,
            in_specs=[hbm, hbm, whole],
            out_specs=(whole, whole),
            scratch_shapes=[
                pltpu.VMEM((3, 2, parts, chunks, width, size), BF16),
                pltpu.VMEM((chunks, width, size), BF16),
                pltpu.VMEM((2, parts, chunks, width, size), BF16),
                pltpu.VMEM((2, parts, rows, width), BF16),
                pltpu.VMEM((2, chunks, 1, size), F32),
                pltpu.VMEM((2, width, rows), F32),
                pltpu.VMEM((2, rows, size), F32),
                pltpu.VMEM((2 * parts, 1, 128), F32),
                dma, dma, dma, dma, dma((steps,)), dma, dma((steps,)), dma, dma((chunks,)),
                dma((parts - 1,)), dma((parts - 1,)),
                dma((parts - 1,)), dma((steps, parts - 1)), pltpu.SemaphoreType.REGULAR,
            ],
            compiler_params=pltpu.CompilerParams(
                collective_id=0, has_side_effects=True, vmem_limit_bytes=VMEM_LIMIT),
        )(image.T, text.T, constant)
        image_grad, text_grad = pl.pallas_call(
            publish,
            out_shape=(out, out),
            in_specs=[anywhere, anywhere],
            out_specs=(hbm, hbm),
            scratch_shapes=[dma((2,))],
            compiler_params=pltpu.CompilerParams(vmem_limit_bytes=4 << 20),
        )(image_grad, text_grad)
        return image_grad.T, text_grad.T

    placed = (P("dp", "mp"), P("dp", "mp"), P(), P(), P())
    return jax.shard_map(
        local, mesh=mesh, in_specs=placed, out_specs=(P("dp", "mp"), P("dp", "mp")), check_vma=False
    )
```

```python
import functools

import jax
import jax.numpy as jnp
from jax import lax
from jax.experimental import pallas as pl
from jax.experimental.pallas import tpu as pltpu
from jax.sharding import PartitionSpec as P

MESH = pl.DeviceIdType.MESH
F32 = jnp.float32
BF16 = jnp.bfloat16
IMAGE, TEXT = 0, 1
VMEM_LIMIT = 60 << 20


def kernel(
    blocks, parts, chunks,
    image_ref, text_ref, constant_ref,
    early_out, unit_out, sums, inner, own_inverse,
    raw, relay, own_unit, own_rows, constants,
    load_sem, constant_send, constant_recv, far_send, far_recv, near_send, near_recv, leg_send, leg_recv,
    own_send, own_recv, share_send, share_recv, token,
):
    width, rows = image_ref.shape
    size = rows // chunks
    steps = 2 * chunks
    me = lax.axis_index("dp")
    part = lax.axis_index("mp")
    parity = lax.rem(me, 2)
    near = me + 1 - 2 * parity
    late = 1 - parity
    row = lax.rem(me // 2, 2)
    relayed = parity != row
    direct = jnp.logical_not(relayed)
    members = 2 * parts
    member = parity * parts + part

    def shifted(by):
        return lax.rem(me + blocks + by, blocks)

    def load(ref, side, index):
        return pltpu.make_async_copy(
            ref.at[:, pl.ds(index * size, size)], raw.at[0, side, 0, index], load_sem)

    for index in range(chunks):
        load(image_ref, IMAGE, index).start()
        load(text_ref, TEXT, index).start()
    constants[member] = constant_ref[...]

    def settle(ref, sem):
        pltpu.make_async_copy(ref, ref, sem).wait()

    def mate(offset):
        other = lax.rem(member + offset, members)
        return {"dp": me - parity + other // parts, "mp": lax.rem(other, parts)}

    def constant_copy(offset):
        return pltpu.make_async_remote_copy(
            src_ref=constant_ref, dst_ref=constants.at[member],
            send_sem=constant_send, recv_sem=constant_recv,
            device_id=mate(offset), device_id_type=MESH)

    def side_of(step):
        return jnp.where(step < chunks, parity, 1 - parity)

    def piece(k, side, slot, step):
        return raw.at[k, side, slot, lax.rem(step, chunks)]

    def far_copy(step):
        side = side_of(step)
        return pltpu.make_async_remote_copy(
            src_ref=piece(0, side, 0, step), dst_ref=piece(2, side, 0, step),
            send_sem=far_send, recv_sem=far_recv.at[step],
            device_id={"dp": shifted(4 * side - 2)}, device_id_type=MESH)

    def leg_copy(index):
        return pltpu.make_async_remote_copy(
            src_ref=raw.at[0, late, 0, index], dst_ref=relay.at[index],
            send_sem=leg_send, recv_sem=leg_recv.at[index],
            device_id={"dp": shifted(8 * late - 4)}, device_id_type=MESH)

    def relay_copy(index):
        return pltpu.make_async_remote_copy(
            src_ref=relay.at[index], dst_ref=raw.at[2, late, 0, index],
            send_sem=far_send, recv_sem=far_recv.at[chunks + index],
            device_id={"dp": shifted(2 - 4 * late)}, device_id_type=MESH)

    def near_copy(step, k):
        side = 1 - side_of(step)
        return pltpu.make_async_remote_copy(
            src_ref=piece(k, side, 0, step), dst_ref=piece(1, side, 0, step),
            send_sem=near_send, recv_sem=near_recv.at[step],
            device_id={"dp": near}, device_id_type=MESH)

    def own_copy(side, offset):
        return pltpu.make_async_remote_copy(
            src_ref=raw.at[0, side, 0], dst_ref=raw.at[0, side, parts - offset],
            send_sem=own_send.at[offset - 1], recv_sem=own_recv.at[parts - offset - 1],
            device_id={"mp": lax.rem(part + offset, parts)}, device_id_type=MESH)

    def share_copy(k, step, offset):
        side = side_of(step)
        return pltpu.make_async_remote_copy(
            src_ref=piece(k, side, 0, step), dst_ref=piece(k, side, parts - offset, step),
            send_sem=share_send.at[offset - 1], recv_sem=share_recv.at[step, parts - offset - 1],
            device_id={"mp": lax.rem(part + offset, parts)}, device_id_type=MESH)

    barrier = pltpu.get_barrier_semaphore()

    def greet(target):
        pl.semaphore_signal(barrier, inc=1, device_id={"dp": target}, device_id_type=MESH)

    greet(shifted(2 - 4 * row))

    @pl.when(relayed)
    def _():
        greet(shifted(-2 - 2 * row))

    for offset in range(1, members):
        pl.semaphore_signal(barrier, inc=1, device_id=mate(offset), device_id_type=MESH)
    settle(raw.at[0, :, 0], load_sem)
    pl.semaphore_wait(barrier, row + members)

    for offset in range(1, members):
        constant_copy(offset).start()

    def inform(target):
        pl.semaphore_signal(token, inc=1, device_id={"dp": target}, device_id_type=MESH)

    @pl.when(row == 1)
    def _():
        inform(shifted(4 - 2 * parity))

    for step in range(chunks):
        @pl.when(parity + row > 0)
        def _():
            far_copy(step).start()

        near_copy(step, 0).start()

    @pl.when(direct)
    def _():
        for step in range(chunks, steps):
            far_copy(step).start()

    for side in (IMAGE, TEXT):
        for offset in range(1, parts):
            own_copy(side, offset).start()

    def unit_rows(k, side, index):
        wide = [raw[k, side, slot, index].astype(F32) for slot in range(parts)]
        square = sum(jnp.sum(w * w, axis=0, keepdims=True) for w in wide)
        inverse = lax.rsqrt(square + 1e-06)
        return [(w * inverse).astype(BF16) for w in wide], inverse

    def pair_terms(units, side, diagonal):
        other = 1 - side
        scale = jnp.exp(constants[0, :, 0:1])
        bias = constants[1, :, 0:1]
        weight = scale * constants[2, :, 0:1]
        total = jnp.dot(own_rows[other], jnp.concatenate(units, axis=0), preferred_element_type=F32)
        scores = scale * total + bias
        if diagonal:
            shape = total.shape
            matching = lax.broadcasted_iota(jnp.int32, shape, 0) == lax.broadcasted_iota(jnp.int32, shape, 1)
            sign = jnp.where(matching, 1.0, -1.0).astype(F32)
            factor = -weight * sign * jax.nn.sigmoid(-sign * scores)
        else:
            factor = weight * jax.nn.sigmoid(scores)
        factor = factor.astype(BF16)
        gradient = lax.dot_general(
            units[0], factor, (((1,), (1,)), ((), ())), preferred_element_type=F32)
        product = factor.astype(F32) * total
        product = sum(product[:, at:at + size] for at in range(0, product.shape[1], size))
        if diagonal:
            sums[other] = gradient
            inner[other] = product
        else:
            sums[other] += gradient
            inner[other] += product

    @pl.when((parity == 0) & (row == 1))
    def _():
        for index in range(chunks):
            leg_copy(index).start()
        pl.semaphore_wait(token, 1)
        inform(shifted(-2))

    @pl.when((parity == 0) & (row == 0))
    def _():
        pl.semaphore_wait(token, 1)
        for step in range(chunks):
            far_copy(step).start()

    @pl.when((parity == 1) & (row == 0))
    def _():
        pl.semaphore_wait(token, 1)
        for index in range(chunks):
            leg_copy(index).start()

    for slot in range(1, parts):
        settle(raw.at[0, :, slot], own_recv.at[slot - 1])

    def own_norm(index, carry):
        side, place = index // chunks, lax.rem(index, chunks)
        units, inverse = unit_rows(0, side, place)
        for slot in range(parts):
            own_unit[side, slot, place] = units[slot]
        own_rows[side, pl.ds(pl.multiple_of(place * size, size), size), :] = jnp.concatenate(units, axis=0).T
        own_inverse[side, place] = inverse
        return carry

    lax.fori_loop(0, steps, own_norm, 0)
    settle(constants.at[pl.ds(1, members - 1)], constant_recv)

    def own_pairs(side, carry):
        pair_terms(
            [jnp.concatenate([own_unit[side, slot, place] for place in range(chunks)], axis=1)
             for slot in range(parts)], side, True)
        return carry

    lax.fori_loop(0, 2, own_pairs, 0)

    def place_of(index):
        return slice(index * size, (index + 1) * size)

    def early_finish():
        for index in range(chunks):
            place = place_of(index)
            early_out[:, place] = finish(
                sums[late, :, place], inner[late, place], own_inverse[late, index],
                raw[0, late, 0, index].astype(F32) * own_inverse[late, index])
            unit_out[:, place] = raw[0, parity, 0, index].astype(F32) * own_inverse[parity, index]

    def advance(step, carry):
        @pl.when(step < steps)
        def _():
            far_copy(step).wait_recv()

            @pl.when(step < chunks)
            def _():
                near_copy(step + chunks, 2).start()

            @pl.when((step < chunks) & relayed)
            def _():
                leg_copy(step).wait_recv()
                relay_copy(step).start()

            for offset in range(1, parts):
                share_copy(2, step, offset).start()
            near_copy(step, 0).wait_recv()
            for offset in range(1, parts):
                share_copy(1, step, offset).start()

        @pl.when(step > 0)
        def _():
            past = step - 1
            side = side_of(past)
            for slot in range(1, parts):
                settle(raw.at[pl.ds(1, 2), side, slot, lax.rem(past, chunks)], share_recv.at[past, slot - 1])
            units = [unit_rows(k, side, lax.rem(past, chunks))[0] for k in (1, 2)]
            pair_terms([jnp.concatenate(halves, axis=1) for halves in zip(*units)], side, False)

        @pl.when(step == chunks)
        def _():
            early_finish()

        return carry

    lax.fori_loop(0, steps + 1, advance, 0)

    @pl.when(relayed)
    def _():
        settle(relay, leg_send)

    settle(raw.at[0, :, 0], far_send)
    settle(raw.at[0, :, 0], near_send)
    settle(constants.at[pl.ds(1, members - 1)], constant_send)
    for offset in range(1, parts):
        settle(raw.at[0, :, 0], own_send.at[offset - 1])
        settle(raw.at[pl.ds(0, 2), :, 0], share_send.at[offset - 1])


def spread(value_ref, row_ref):
    row_ref[...] = jnp.full(row_ref.shape, value_ref[0])


def finish(gradient, products, inverse, unit):
    inner = jnp.sum(products.T, axis=0, keepdims=True)
    return inverse * (gradient - unit * inner)


def publish(early_ref, unit_ref, sums, inner, own_inverse, image_out, text_out, late_ref, early_sem, late_sem):
    parity = lax.rem(lax.axis_index("dp"), 2)
    chunks, _, size = own_inverse.shape[1:]

    def emit(first, second, ref, place, sem):
        @pl.when(parity == 0)
        def _():
            pltpu.make_async_copy(ref.at[:, place], first.at[:, place], sem).start()

        @pl.when(parity == 1)
        def _():
            pltpu.make_async_copy(ref.at[:, place], second.at[:, place], sem).start()

    emit(text_out, image_out, early_ref, slice(None), early_sem)
    for index in range(chunks):
        place = slice(index * size, (index + 1) * size)
        late_ref[:, place] = finish(
            sums[parity, :, place], inner[parity, place], own_inverse[parity, index], unit_ref[:, place])
        emit(image_out, text_out, late_ref, place, late_sem)
    pltpu.make_async_copy(early_ref, early_ref, early_sem).wait()
    pltpu.make_async_copy(late_ref, late_ref, late_sem).wait()


def solution(mesh):
    blocks, parts = mesh.shape["dp"], mesh.shape["mp"]

    def local(image, text, log_logit_scale, bias, loss_upstream_gradient):
        rows, width = image.shape
        chunks = max(rows // 128, 1)
        size = rows // chunks
        steps = 2 * chunks
        hbm = pl.BlockSpec(memory_space=pltpu.HBM)
        whole = pl.BlockSpec(memory_space=pltpu.VMEM)
        dma = pltpu.SemaphoreType.DMA
        out = jax.ShapeDtypeStruct((width, rows), F32)
        member = lax.rem(lax.axis_index("dp"), 2) * parts + lax.axis_index("mp")

        def pick(place):
            def branch(*values):
                return pl.pallas_call(
                    spread,
                    out_shape=pltpu.VMEM((1, 128), F32),
                    in_specs=[pl.BlockSpec(memory_space=pltpu.SMEM)],
                    out_specs=whole,
                    name=f"constant_{place}",
                    compiler_params=pltpu.CompilerParams(vmem_limit_bytes=1 << 20),
                )(values[place].reshape(1))
            return branch

        constant = lax.switch(
            lax.rem(member, 3), [pick(place) for place in range(3)], log_logit_scale, bias, loss_upstream_gradient)
        results = pl.pallas_call(
            functools.partial(kernel, blocks, parts, chunks),
            out_shape=(
                pltpu.VMEM((width, rows), F32), pltpu.VMEM((width, rows), F32),
                pltpu.VMEM((2, width, rows), F32), pltpu.VMEM((2, rows, size), F32),
                pltpu.VMEM((2, chunks, 1, size), F32)),
            in_specs=[hbm, hbm, whole],
            out_specs=(whole,) * 5,
            scratch_shapes=[
                pltpu.VMEM((3, 2, parts, chunks, width, size), BF16),
                pltpu.VMEM((chunks, width, size), BF16),
                pltpu.VMEM((2, parts, chunks, width, size), BF16),
                pltpu.VMEM((2, rows, parts * width), BF16),
                pltpu.VMEM((2 * parts, 1, 128), F32),
                dma, dma, dma, dma, dma((steps,)), dma, dma((steps,)), dma, dma((chunks,)),
                dma((parts - 1,)), dma((parts - 1,)),
                dma((parts - 1,)), dma((steps, parts - 1)), pltpu.SemaphoreType.REGULAR,
            ],
            compiler_params=pltpu.CompilerParams(
                collective_id=0, has_side_effects=True, vmem_limit_bytes=VMEM_LIMIT),
        )(image.T, text.T, constant)
        image_grad, text_grad = pl.pallas_call(
            publish,
            out_shape=(out, out),
            in_specs=[whole] * 5,
            out_specs=(hbm, hbm),
            scratch_shapes=[pltpu.VMEM((width, rows), F32), dma, dma],
            compiler_params=pltpu.CompilerParams(vmem_limit_bytes=16 << 20),
        )(*results)
        return image_grad.T, text_grad.T

    placed = (P("dp", "mp"), P("dp", "mp"), P(), P(), P())
    return jax.shard_map(
        local, mesh=mesh, in_specs=placed, out_specs=(P("dp", "mp"), P("dp", "mp")), check_vma=False
    )
```

```python
import functools

import jax
import jax.numpy as jnp
from jax import lax
from jax.experimental import pallas as pl
from jax.experimental.pallas import tpu as pltpu
from jax.sharding import PartitionSpec as P

MESH = pl.DeviceIdType.MESH
F32 = jnp.float32
BF16 = jnp.bfloat16
IMAGE, TEXT = 0, 1
VMEM_LIMIT = 60 << 20


def kernel(
    blocks, parts, chunks,
    image_ref, text_ref, constant_ref,
    early_out, unit_out, sums, inner, own_inverse,
    raw, relay, own_unit, own_rows, constants,
    load_sem, constant_send, constant_recv, far_send, far_recv, near_send, near_recv, leg_send, leg_recv,
    own_send, own_recv, share_send, share_recv, token,
):
    width, rows = image_ref.shape
    size = rows // chunks
    steps = 2 * chunks
    me = lax.axis_index("dp")
    part = lax.axis_index("mp")
    parity = lax.rem(me, 2)
    near = me + 1 - 2 * parity
    late = 1 - parity
    row = lax.rem(me // 2, 2)
    relayed = parity != row
    direct = jnp.logical_not(relayed)
    members = 2 * parts
    final = steps - 1
    beside = lax.rem(part + 1, parts)
    member = parity * parts + part

    def shifted(by):
        return lax.rem(me + blocks + by, blocks)

    def load(ref, side, index):
        return pltpu.make_async_copy(
            ref.at[:, pl.ds(index * size, size)], raw.at[0, side, 0, index], load_sem)

    for index in range(chunks):
        load(image_ref, IMAGE, index).start()
        load(text_ref, TEXT, index).start()
    constants[member] = constant_ref[...]

    def settle(ref, sem):
        pltpu.make_async_copy(ref, ref, sem).wait()

    def mate(offset):
        other = lax.rem(member + offset, members)
        return {"dp": me - parity + other // parts, "mp": lax.rem(other, parts)}

    def constant_copy(offset):
        return pltpu.make_async_remote_copy(
            src_ref=constant_ref, dst_ref=constants.at[member],
            send_sem=constant_send, recv_sem=constant_recv,
            device_id=mate(offset), device_id_type=MESH)

    def side_of(step):
        return jnp.where(step < chunks, parity, 1 - parity)

    def landing(step):
        return jnp.where(step == final, parts - 1, 0)

    def lander(step):
        return jnp.where(step == final, beside, part)

    def piece(k, side, slot, step):
        return raw.at[k, side, slot, lax.rem(step, chunks)]

    def far_copy(step):
        side = side_of(step)
        return pltpu.make_async_remote_copy(
            src_ref=piece(0, side, 0, step), dst_ref=piece(2, side, landing(step), step),
            send_sem=far_send, recv_sem=far_recv.at[step],
            device_id={"dp": shifted(4 * side - 2), "mp": lander(step)}, device_id_type=MESH)

    def leg_copy(index):
        return pltpu.make_async_remote_copy(
            src_ref=raw.at[0, late, 0, index], dst_ref=relay.at[index],
            send_sem=leg_send, recv_sem=leg_recv.at[index],
            device_id={"dp": shifted(8 * late - 4)}, device_id_type=MESH)

    def relay_copy(index):
        return pltpu.make_async_remote_copy(
            src_ref=relay.at[index], dst_ref=raw.at[2, late, landing(chunks + index), index],
            send_sem=far_send, recv_sem=far_recv.at[chunks + index],
            device_id={"dp": shifted(2 - 4 * late), "mp": lander(chunks + index)}, device_id_type=MESH)

    def near_copy(step, k):
        side = 1 - side_of(step)
        return pltpu.make_async_remote_copy(
            src_ref=piece(k, side, 0, step), dst_ref=piece(1, side, landing(step), step),
            send_sem=near_send, recv_sem=near_recv.at[step],
            device_id={"dp": near, "mp": lander(step)}, device_id_type=MESH)

    def own_copy(side, offset):
        return pltpu.make_async_remote_copy(
            src_ref=raw.at[0, side, 0], dst_ref=raw.at[0, side, parts - offset],
            send_sem=own_send.at[offset - 1], recv_sem=own_recv.at[parts - offset - 1],
            device_id={"mp": lax.rem(part + offset, parts)}, device_id_type=MESH)

    def share_copy(k, step, offset):
        side = side_of(step)
        return pltpu.make_async_remote_copy(
            src_ref=piece(k, side, landing(step), step),
            dst_ref=piece(k, side, parts - offset - jnp.where(step == final, 1, 0), step),
            send_sem=share_send.at[offset - 1], recv_sem=share_recv.at[step, parts - offset - 1],
            device_id={"mp": lax.rem(part + offset, parts)}, device_id_type=MESH)

    barrier = pltpu.get_barrier_semaphore()

    def greet(target):
        pl.semaphore_signal(barrier, inc=1, device_id={"dp": target}, device_id_type=MESH)

    greet(shifted(2 - 4 * row))
    pl.semaphore_signal(
        barrier, inc=1, device_id={"dp": shifted(2 - 4 * row), "mp": lax.rem(part + parts - 1, parts)},
        device_id_type=MESH)

    @pl.when(relayed)
    def _():
        greet(shifted(-2 - 2 * row))

    for offset in range(1, members):
        pl.semaphore_signal(barrier, inc=1, device_id=mate(offset), device_id_type=MESH)
    settle(raw.at[0, :, 0], load_sem)
    pl.semaphore_wait(barrier, 1 + row + members)

    for offset in range(1, members):
        constant_copy(offset).start()

    def inform(target):
        pl.semaphore_signal(token, inc=1, device_id={"dp": target}, device_id_type=MESH)

    @pl.when(row == 1)
    def _():
        inform(shifted(4 - 2 * parity))

    for step in range(chunks):
        @pl.when(parity + row > 0)
        def _():
            far_copy(step).start()

        near_copy(step, 0).start()

    @pl.when(direct)
    def _():
        for step in range(chunks, steps):
            far_copy(step).start()

    for side in (IMAGE, TEXT):
        for offset in range(1, parts):
            own_copy(side, offset).start()

    def unit_rows(k, side, index):
        wide = [raw[k, side, slot, index].astype(F32) for slot in range(parts)]
        square = sum(jnp.sum(w * w, axis=0, keepdims=True) for w in wide)
        inverse = lax.rsqrt(square + 1e-06)
        return [(w * inverse).astype(BF16) for w in wide], inverse

    def pair_terms(units, side, diagonal):
        other = 1 - side
        scale = jnp.exp(constants[0, :, 0:1])
        bias = constants[1, :, 0:1]
        weight = scale * constants[2, :, 0:1]
        total = jnp.dot(own_rows[other], jnp.concatenate(units, axis=0), preferred_element_type=F32)
        scores = scale * total + bias
        if diagonal:
            shape = total.shape
            matching = lax.broadcasted_iota(jnp.int32, shape, 0) == lax.broadcasted_iota(jnp.int32, shape, 1)
            sign = jnp.where(matching, 1.0, -1.0).astype(F32)
            factor = -weight * sign * jax.nn.sigmoid(-sign * scores)
        else:
            factor = weight * jax.nn.sigmoid(scores)
        factor = factor.astype(BF16)
        gradient = lax.dot_general(
            units[0], factor, (((1,), (1,)), ((), ())), preferred_element_type=F32)
        product = factor.astype(F32) * total
        product = sum(product[:, at:at + size] for at in range(0, product.shape[1], size))
        if diagonal:
            sums[other] = gradient
            inner[other] = product
        else:
            sums[other] += gradient
            inner[other] += product

    @pl.when((parity == 0) & (row == 1))
    def _():
        for index in range(chunks):
            leg_copy(index).start()
        pl.semaphore_wait(token, 1)
        inform(shifted(-2))

    @pl.when((parity == 0) & (row == 0))
    def _():
        pl.semaphore_wait(token, 1)
        for step in range(chunks):
            far_copy(step).start()

    @pl.when((parity == 1) & (row == 0))
    def _():
        pl.semaphore_wait(token, 1)
        for index in range(chunks):
            leg_copy(index).start()

    for slot in range(1, parts):
        settle(raw.at[0, :, slot], own_recv.at[slot - 1])

    def own_norm(index, carry):
        side, place = index // chunks, lax.rem(index, chunks)
        units, inverse = unit_rows(0, side, place)
        for slot in range(parts):
            own_unit[side, slot, place] = units[slot]
        own_rows[side, pl.ds(pl.multiple_of(place * size, size), size), :] = jnp.concatenate(units, axis=0).T
        own_inverse[side, place] = inverse
        return carry

    lax.fori_loop(0, steps, own_norm, 0)
    settle(constants.at[pl.ds(1, members - 1)], constant_recv)

    def own_pairs(side, carry):
        pair_terms(
            [jnp.concatenate([own_unit[side, slot, place] for place in range(chunks)], axis=1)
             for slot in range(parts)], side, True)
        return carry

    lax.fori_loop(0, 2, own_pairs, 0)

    def place_of(index):
        return slice(index * size, (index + 1) * size)

    def early_finish():
        for index in range(chunks):
            place = place_of(index)
            early_out[:, place] = finish(
                sums[late, :, place], inner[late, place], own_inverse[late, index],
                raw[0, late, 0, index].astype(F32) * own_inverse[late, index])
            unit_out[:, place] = raw[0, parity, 0, index].astype(F32) * own_inverse[parity, index]

    def advance(step, carry):
        @pl.when(step < steps)
        def _():
            far_copy(step).wait_recv()

            @pl.when(step < chunks)
            def _():
                near_copy(step + chunks, 2).start()

            @pl.when((step < chunks) & relayed)
            def _():
                leg_copy(step).wait_recv()
                relay_copy(step).start()

            for offset in range(1, parts):
                share_copy(2, step, offset).start()
            near_copy(step, 0).wait_recv()
            for offset in range(1, parts):
                share_copy(1, step, offset).start()

        @pl.when(step > 0)
        def _():
            past = step - 1
            side = side_of(past)
            for slot in range(1, parts):
                settle(raw.at[pl.ds(1, 2), side, slot, lax.rem(past, chunks)], share_recv.at[past, slot - 1])
            units = [unit_rows(k, side, lax.rem(past, chunks))[0] for k in (1, 2)]
            pair_terms([jnp.concatenate(halves, axis=1) for halves in zip(*units)], side, False)

        @pl.when(step == chunks)
        def _():
            early_finish()

        return carry

    lax.fori_loop(0, steps + 1, advance, 0)

    @pl.when(relayed)
    def _():
        settle(relay, leg_send)

    settle(raw.at[0, :, 0], far_send)
    settle(raw.at[0, :, 0], near_send)
    settle(constants.at[pl.ds(1, members - 1)], constant_send)
    for offset in range(1, parts):
        settle(raw.at[0, :, 0], own_send.at[offset - 1])
        settle(raw.at[pl.ds(0, 2), :, 0], share_send.at[offset - 1])


def spread(value_ref, row_ref):
    row_ref[...] = jnp.full(row_ref.shape, value_ref[0])


def finish(gradient, products, inverse, unit):
    inner = jnp.sum(products.T, axis=0, keepdims=True)
    return inverse * (gradient - unit * inner)


def publish(early_ref, unit_ref, sums, inner, own_inverse, image_out, text_out, late_ref, early_sem, late_sem):
    parity = lax.rem(lax.axis_index("dp"), 2)
    chunks, _, size = own_inverse.shape[1:]

    def emit(first, second, ref, place, sem):
        @pl.when(parity == 0)
        def _():
            pltpu.make_async_copy(ref.at[:, place], first.at[:, place], sem).start()

        @pl.when(parity == 1)
        def _():
            pltpu.make_async_copy(ref.at[:, place], second.at[:, place], sem).start()

    emit(text_out, image_out, early_ref, slice(None), early_sem)
    for index in range(chunks):
        place = slice(index * size, (index + 1) * size)
        late_ref[:, place] = finish(
            sums[parity, :, place], inner[parity, place], own_inverse[parity, index], unit_ref[:, place])
        emit(image_out, text_out, late_ref, place, late_sem)
    pltpu.make_async_copy(early_ref, early_ref, early_sem).wait()
    pltpu.make_async_copy(late_ref, late_ref, late_sem).wait()


def solution(mesh):
    blocks, parts = mesh.shape["dp"], mesh.shape["mp"]

    def local(image, text, log_logit_scale, bias, loss_upstream_gradient):
        rows, width = image.shape
        chunks = max(rows // 128, 1)
        size = rows // chunks
        steps = 2 * chunks
        hbm = pl.BlockSpec(memory_space=pltpu.HBM)
        whole = pl.BlockSpec(memory_space=pltpu.VMEM)
        dma = pltpu.SemaphoreType.DMA
        out = jax.ShapeDtypeStruct((width, rows), F32)
        member = lax.rem(lax.axis_index("dp"), 2) * parts + lax.axis_index("mp")

        def pick(place):
            def branch(*values):
                return pl.pallas_call(
                    spread,
                    out_shape=pltpu.VMEM((1, 128), F32),
                    in_specs=[pl.BlockSpec(memory_space=pltpu.SMEM)],
                    out_specs=whole,
                    name=f"constant_{place}",
                    compiler_params=pltpu.CompilerParams(vmem_limit_bytes=1 << 20),
                )(values[place].reshape(1))
            return branch

        constant = lax.switch(
            lax.rem(member, 3), [pick(place) for place in range(3)], log_logit_scale, bias, loss_upstream_gradient)
        results = pl.pallas_call(
            functools.partial(kernel, blocks, parts, chunks),
            out_shape=(
                pltpu.VMEM((width, rows), F32), pltpu.VMEM((width, rows), F32),
                pltpu.VMEM((2, width, rows), F32), pltpu.VMEM((2, rows, size), F32),
                pltpu.VMEM((2, chunks, 1, size), F32)),
            in_specs=[hbm, hbm, whole],
            out_specs=(whole,) * 5,
            scratch_shapes=[
                pltpu.VMEM((3, 2, parts, chunks, width, size), BF16),
                pltpu.VMEM((chunks, width, size), BF16),
                pltpu.VMEM((2, parts, chunks, width, size), BF16),
                pltpu.VMEM((2, rows, parts * width), BF16),
                pltpu.VMEM((2 * parts, 1, 128), F32),
                dma, dma, dma, dma, dma((steps,)), dma, dma((steps,)), dma, dma((chunks,)),
                dma((parts - 1,)), dma((parts - 1,)),
                dma((parts - 1,)), dma((steps, parts - 1)), pltpu.SemaphoreType.REGULAR,
            ],
            compiler_params=pltpu.CompilerParams(
                collective_id=0, has_side_effects=True, vmem_limit_bytes=VMEM_LIMIT),
        )(image.T, text.T, constant)
        image_grad, text_grad = pl.pallas_call(
            publish,
            out_shape=(out, out),
            in_specs=[whole] * 5,
            out_specs=(hbm, hbm),
            scratch_shapes=[pltpu.VMEM((width, rows), F32), dma, dma],
            compiler_params=pltpu.CompilerParams(vmem_limit_bytes=16 << 20),
        )(*results)
        return image_grad.T, text_grad.T

    placed = (P("dp", "mp"), P("dp", "mp"), P(), P(), P())
    return jax.shard_map(
        local, mesh=mesh, in_specs=placed, out_specs=(P("dp", "mp"), P("dp", "mp")), check_vma=False
    )
```

```python
import functools

import jax
import jax.numpy as jnp
from jax import lax
from jax.experimental import pallas as pl
from jax.experimental.pallas import tpu as pltpu
from jax.sharding import PartitionSpec as P

MESH = pl.DeviceIdType.MESH
F32 = jnp.float32
BF16 = jnp.bfloat16
IMAGE, TEXT = 0, 1
VMEM_LIMIT = 60 << 20


def kernel(
    blocks, parts, chunks,
    image_ref, text_ref, constant_ref,
    early_out, unit_out, sums, inner, own_inverse,
    raw, relay, own_unit, own_rows, constants,
    load_sem, constant_send, constant_recv, far_send, far_recv, near_send, near_recv, leg_send, leg_recv,
    own_send, own_recv, share_send, share_recv, token,
):
    width, rows = image_ref.shape
    size = rows // chunks
    steps = 2 * chunks
    me = lax.axis_index("dp")
    part = lax.axis_index("mp")
    parity = lax.rem(me, 2)
    near = me + 1 - 2 * parity
    late = 1 - parity
    row = lax.rem(me // 2, 2)
    relayed = parity != row
    direct = jnp.logical_not(relayed)
    members = 2 * parts
    end, final = chunks - 1, steps - 1
    half = width // 2
    beside = lax.rem(part + 1, parts)
    member = parity * parts + part

    def shifted(by):
        return lax.rem(me + blocks + by, blocks)

    def load(ref, side, index):
        return pltpu.make_async_copy(
            ref.at[:, pl.ds(index * size, size)], raw.at[0, side, 0, index], load_sem)

    for index in range(chunks):
        load(image_ref, IMAGE, index).start()
        load(text_ref, TEXT, index).start()
    constants[member] = constant_ref[...]

    def settle(ref, sem):
        pltpu.make_async_copy(ref, ref, sem).wait()

    def mate(offset):
        other = lax.rem(member + offset, members)
        return {"dp": me - parity + other // parts, "mp": lax.rem(other, parts)}

    def constant_copy(offset):
        return pltpu.make_async_remote_copy(
            src_ref=constant_ref, dst_ref=constants.at[member],
            send_sem=constant_send, recv_sem=constant_recv,
            device_id=mate(offset), device_id_type=MESH)

    def side_of(step):
        return jnp.where(step < chunks, parity, 1 - parity)

    def piece(k, side, slot, step):
        return raw.at[k, side, slot, lax.rem(step, chunks)]

    def far_copy(step):
        side = side_of(step)
        return pltpu.make_async_remote_copy(
            src_ref=piece(0, side, 0, step), dst_ref=piece(2, side, 0, step),
            send_sem=far_send, recv_sem=far_recv.at[step],
            device_id={"dp": shifted(4 * side - 2)}, device_id_type=MESH)

    def leg_copy(index):
        return pltpu.make_async_remote_copy(
            src_ref=raw.at[0, late, 0, index], dst_ref=relay.at[index],
            send_sem=leg_send, recv_sem=leg_recv.at[index],
            device_id={"dp": shifted(8 * late - 4)}, device_id_type=MESH)

    def relay_copy(index):
        return pltpu.make_async_remote_copy(
            src_ref=relay.at[index], dst_ref=raw.at[2, late, 0, index],
            send_sem=far_send, recv_sem=far_recv.at[chunks + index],
            device_id={"dp": shifted(2 - 4 * late)}, device_id_type=MESH)

    def near_copy(step, k):
        side = 1 - side_of(step)
        return pltpu.make_async_remote_copy(
            src_ref=piece(k, side, 0, step), dst_ref=piece(1, side, 0, step),
            send_sem=near_send, recv_sem=near_recv.at[step],
            device_id={"dp": near}, device_id_type=MESH)

    def end_piece(k, side, slot, cut):
        return raw.at[k, side, slot, end, pl.ds(cut * half, half)]

    def far_end(cut):
        return pltpu.make_async_remote_copy(
            src_ref=end_piece(0, late, 0, cut), dst_ref=end_piece(2, late, parts - 1, cut),
            send_sem=far_send, recv_sem=far_recv.at[final + cut],
            device_id={"dp": shifted(4 * late - 2), "mp": beside}, device_id_type=MESH)

    def relay_end(cut):
        return pltpu.make_async_remote_copy(
            src_ref=relay.at[end, pl.ds(cut * half, half)], dst_ref=end_piece(2, late, parts - 1, cut),
            send_sem=far_send, recv_sem=far_recv.at[final + cut],
            device_id={"dp": shifted(2 - 4 * late), "mp": beside}, device_id_type=MESH)

    def near_end(cut):
        return pltpu.make_async_remote_copy(
            src_ref=end_piece(2, parity, 0, cut), dst_ref=end_piece(1, parity, parts - 1, cut),
            send_sem=near_send, recv_sem=near_recv.at[final + cut],
            device_id={"dp": near, "mp": beside}, device_id_type=MESH)

    def share_end(k, cut, offset):
        return pltpu.make_async_remote_copy(
            src_ref=end_piece(k, late, parts - 1, cut), dst_ref=end_piece(k, late, parts - 1 - offset, cut),
            send_sem=share_send.at[offset - 1], recv_sem=share_recv.at[final, parts - offset - 1],
            device_id={"mp": lax.rem(part + offset, parts)}, device_id_type=MESH)

    def own_copy(side, offset):
        return pltpu.make_async_remote_copy(
            src_ref=raw.at[0, side, 0], dst_ref=raw.at[0, side, parts - offset],
            send_sem=own_send.at[offset - 1], recv_sem=own_recv.at[parts - offset - 1],
            device_id={"mp": lax.rem(part + offset, parts)}, device_id_type=MESH)

    def share_copy(k, step, offset):
        side = side_of(step)
        return pltpu.make_async_remote_copy(
            src_ref=piece(k, side, 0, step), dst_ref=piece(k, side, parts - offset, step),
            send_sem=share_send.at[offset - 1], recv_sem=share_recv.at[step, parts - offset - 1],
            device_id={"mp": lax.rem(part + offset, parts)}, device_id_type=MESH)

    barrier = pltpu.get_barrier_semaphore()

    def greet(target):
        pl.semaphore_signal(barrier, inc=1, device_id={"dp": target}, device_id_type=MESH)

    greet(shifted(2 - 4 * row))
    pl.semaphore_signal(
        barrier, inc=1, device_id={"dp": shifted(2 - 4 * row), "mp": lax.rem(part + parts - 1, parts)},
        device_id_type=MESH)

    @pl.when(relayed)
    def _():
        greet(shifted(-2 - 2 * row))

    for offset in range(1, members):
        pl.semaphore_signal(barrier, inc=1, device_id=mate(offset), device_id_type=MESH)
    settle(raw.at[0, :, 0], load_sem)
    pl.semaphore_wait(barrier, 1 + row + members)

    for offset in range(1, members):
        constant_copy(offset).start()

    def inform(target):
        pl.semaphore_signal(token, inc=1, device_id={"dp": target}, device_id_type=MESH)

    @pl.when(row == 1)
    def _():
        inform(shifted(4 - 2 * parity))

    for step in range(chunks):
        @pl.when(parity + row > 0)
        def _():
            far_copy(step).start()

        near_copy(step, 0).start()

    @pl.when(direct)
    def _():
        for step in range(chunks, final):
            far_copy(step).start()
        for cut in (0, 1):
            far_end(cut).start()

    for side in (IMAGE, TEXT):
        for offset in range(1, parts):
            own_copy(side, offset).start()

    def unit_rows(k, side, index):
        wide = [raw[k, side, slot, index].astype(F32) for slot in range(parts)]
        square = sum(jnp.sum(w * w, axis=0, keepdims=True) for w in wide)
        inverse = lax.rsqrt(square + 1e-06)
        return [(w * inverse).astype(BF16) for w in wide], inverse

    def pair_terms(units, side, diagonal):
        other = 1 - side
        scale = jnp.exp(constants[0, :, 0:1])
        bias = constants[1, :, 0:1]
        weight = scale * constants[2, :, 0:1]
        total = jnp.dot(own_rows[other], jnp.concatenate(units, axis=0), preferred_element_type=F32)
        scores = scale * total + bias
        if diagonal:
            shape = total.shape
            matching = lax.broadcasted_iota(jnp.int32, shape, 0) == lax.broadcasted_iota(jnp.int32, shape, 1)
            sign = jnp.where(matching, 1.0, -1.0).astype(F32)
            factor = -weight * sign * jax.nn.sigmoid(-sign * scores)
        else:
            factor = weight * jax.nn.sigmoid(scores)
        factor = factor.astype(BF16)
        gradient = lax.dot_general(
            units[0], factor, (((1,), (1,)), ((), ())), preferred_element_type=F32)
        product = factor.astype(F32) * total
        product = sum(product[:, at:at + size] for at in range(0, product.shape[1], size))
        if diagonal:
            sums[other] = gradient
            inner[other] = product
        else:
            sums[other] += gradient
            inner[other] += product

    @pl.when((parity == 0) & (row == 1))
    def _():
        for index in range(chunks):
            leg_copy(index).start()
        pl.semaphore_wait(token, 1)
        inform(shifted(-2))

    @pl.when((parity == 0) & (row == 0))
    def _():
        pl.semaphore_wait(token, 1)
        for step in range(chunks):
            far_copy(step).start()

    @pl.when((parity == 1) & (row == 0))
    def _():
        pl.semaphore_wait(token, 1)
        for index in range(chunks):
            leg_copy(index).start()

    for slot in range(1, parts):
        settle(raw.at[0, :, slot], own_recv.at[slot - 1])

    def own_norm(index, carry):
        side, place = index // chunks, lax.rem(index, chunks)
        units, inverse = unit_rows(0, side, place)
        for slot in range(parts):
            own_unit[side, slot, place] = units[slot]
        own_rows[side, pl.ds(pl.multiple_of(place * size, size), size), :] = jnp.concatenate(units, axis=0).T
        own_inverse[side, place] = inverse
        return carry

    lax.fori_loop(0, steps, own_norm, 0)
    settle(constants.at[pl.ds(1, members - 1)], constant_recv)

    def own_pairs(side, carry):
        pair_terms(
            [jnp.concatenate([own_unit[side, slot, place] for place in range(chunks)], axis=1)
             for slot in range(parts)], side, True)
        return carry

    lax.fori_loop(0, 2, own_pairs, 0)

    def place_of(index):
        return slice(index * size, (index + 1) * size)

    def early_finish():
        for index in range(chunks):
            place = place_of(index)
            early_out[:, place] = finish(
                sums[late, :, place], inner[late, place], own_inverse[late, index],
                raw[0, late, 0, index].astype(F32) * own_inverse[late, index])
            unit_out[:, place] = raw[0, parity, 0, index].astype(F32) * own_inverse[parity, index]

    def band_pairs(step):
        side = side_of(step)
        for slot in range(1, parts):
            settle(raw.at[pl.ds(1, 2), side, slot, lax.rem(step, chunks)], share_recv.at[step, slot - 1])
        units = [unit_rows(k, side, lax.rem(step, chunks))[0] for k in (1, 2)]
        pair_terms([jnp.concatenate(halves, axis=1) for halves in zip(*units)], side, False)

    def arrive(step):
        far_copy(step).wait_recv()

        @pl.when(step < end)
        def _():
            near_copy(step + chunks, 2).start()

        @pl.when(step == end)
        def _():
            for cut in (0, 1):
                near_end(cut).start()

        @pl.when((step < chunks) & relayed)
        def _():
            leg_copy(step).wait_recv()

            @pl.when(step < end)
            def _():
                relay_copy(step).start()

            @pl.when(step == end)
            def _():
                for cut in (0, 1):
                    relay_end(cut).start()

        for offset in range(1, parts):
            share_copy(2, step, offset).start()
        near_copy(step, 0).wait_recv()
        for offset in range(1, parts):
            share_copy(1, step, offset).start()

    def arrive_end():
        for cut in (0, 1):
            far_end(cut).wait_recv()
            for offset in range(1, parts):
                share_end(2, cut, offset).start()
            near_end(cut).wait_recv()
            for offset in range(1, parts):
                share_end(1, cut, offset).start()

    def advance(step, carry):
        @pl.when(step < final)
        def _():
            arrive(step)

        @pl.when(step == final)
        def _():
            arrive_end()

        @pl.when(step > 0)
        def _():
            band_pairs(step - 1)

        @pl.when(step == chunks)
        def _():
            early_finish()

        return carry

    lax.fori_loop(0, steps + 1, advance, 0)

    @pl.when(relayed)
    def _():
        settle(relay, leg_send)

    settle(raw.at[0, :, 0], far_send)
    settle(raw.at[0, :, 0], near_send)
    settle(constants.at[pl.ds(1, members - 1)], constant_send)
    for offset in range(1, parts):
        settle(raw.at[0, :, 0], own_send.at[offset - 1])
        settle(raw.at[pl.ds(0, 2), :, 0], share_send.at[offset - 1])


def spread(value_ref, row_ref):
    row_ref[...] = jnp.full(row_ref.shape, value_ref[0])


def finish(gradient, products, inverse, unit):
    inner = jnp.sum(products.T, axis=0, keepdims=True)
    return inverse * (gradient - unit * inner)


def publish(early_ref, unit_ref, sums, inner, own_inverse, image_out, text_out, late_ref, early_sem, late_sem):
    parity = lax.rem(lax.axis_index("dp"), 2)
    chunks, _, size = own_inverse.shape[1:]

    def emit(first, second, ref, place, sem):
        @pl.when(parity == 0)
        def _():
            pltpu.make_async_copy(ref.at[:, place], first.at[:, place], sem).start()

        @pl.when(parity == 1)
        def _():
            pltpu.make_async_copy(ref.at[:, place], second.at[:, place], sem).start()

    emit(text_out, image_out, early_ref, slice(None), early_sem)
    for index in range(chunks):
        place = slice(index * size, (index + 1) * size)
        late_ref[:, place] = finish(
            sums[parity, :, place], inner[parity, place], own_inverse[parity, index], unit_ref[:, place])
        emit(image_out, text_out, late_ref, place, late_sem)
    pltpu.make_async_copy(early_ref, early_ref, early_sem).wait()
    pltpu.make_async_copy(late_ref, late_ref, late_sem).wait()


def solution(mesh):
    blocks, parts = mesh.shape["dp"], mesh.shape["mp"]

    def local(image, text, log_logit_scale, bias, loss_upstream_gradient):
        rows, width = image.shape
        chunks = max(rows // 128, 1)
        size = rows // chunks
        steps = 2 * chunks
        hbm = pl.BlockSpec(memory_space=pltpu.HBM)
        whole = pl.BlockSpec(memory_space=pltpu.VMEM)
        dma = pltpu.SemaphoreType.DMA
        out = jax.ShapeDtypeStruct((width, rows), F32)
        member = lax.rem(lax.axis_index("dp"), 2) * parts + lax.axis_index("mp")

        def pick(place):
            def branch(*values):
                return pl.pallas_call(
                    spread,
                    out_shape=pltpu.VMEM((1, 128), F32),
                    in_specs=[pl.BlockSpec(memory_space=pltpu.SMEM)],
                    out_specs=whole,
                    name=f"constant_{place}",
                    compiler_params=pltpu.CompilerParams(vmem_limit_bytes=1 << 20),
                )(values[place].reshape(1))
            return branch

        constant = lax.switch(
            lax.rem(member, 3), [pick(place) for place in range(3)], log_logit_scale, bias, loss_upstream_gradient)
        results = pl.pallas_call(
            functools.partial(kernel, blocks, parts, chunks),
            out_shape=(
                pltpu.VMEM((width, rows), F32), pltpu.VMEM((width, rows), F32),
                pltpu.VMEM((2, width, rows), F32), pltpu.VMEM((2, rows, size), F32),
                pltpu.VMEM((2, chunks, 1, size), F32)),
            in_specs=[hbm, hbm, whole],
            out_specs=(whole,) * 5,
            scratch_shapes=[
                pltpu.VMEM((3, 2, parts, chunks, width, size), BF16),
                pltpu.VMEM((chunks, width, size), BF16),
                pltpu.VMEM((2, parts, chunks, width, size), BF16),
                pltpu.VMEM((2, rows, parts * width), BF16),
                pltpu.VMEM((2 * parts, 1, 128), F32),
                dma, dma, dma, dma, dma((steps + 1,)), dma, dma((steps + 1,)), dma, dma((chunks,)),
                dma((parts - 1,)), dma((parts - 1,)),
                dma((parts - 1,)), dma((steps, parts - 1)), pltpu.SemaphoreType.REGULAR,
            ],
            compiler_params=pltpu.CompilerParams(
                collective_id=0, has_side_effects=True, vmem_limit_bytes=VMEM_LIMIT),
        )(image.T, text.T, constant)
        image_grad, text_grad = pl.pallas_call(
            publish,
            out_shape=(out, out),
            in_specs=[whole] * 5,
            out_specs=(hbm, hbm),
            scratch_shapes=[pltpu.VMEM((width, rows), F32), dma, dma],
            compiler_params=pltpu.CompilerParams(vmem_limit_bytes=16 << 20),
        )(*results)
        return image_grad.T, text_grad.T

    placed = (P("dp", "mp"), P("dp", "mp"), P(), P(), P())
    return jax.shard_map(
        local, mesh=mesh, in_specs=placed, out_specs=(P("dp", "mp"), P("dp", "mp")), check_vma=False
    )
```

```python
import functools

import jax
import jax.numpy as jnp
from jax import lax
from jax.experimental import pallas as pl
from jax.experimental.pallas import tpu as pltpu
from jax.sharding import PartitionSpec as P

MESH = pl.DeviceIdType.MESH
F32 = jnp.float32
BF16 = jnp.bfloat16
IMAGE, TEXT = 0, 1
VMEM_LIMIT = 60 << 20


def kernel(
    blocks, parts, chunks,
    image_ref, text_ref, constant_ref,
    early_out, unit_out, sums, inner, own_inverse,
    raw, relay, own_unit, own_rows, constants,
    load_sem, constant_send, constant_recv, far_send, far_recv, near_send, near_recv, leg_send, leg_recv,
    own_send, own_recv, share_send, share_recv, token,
):
    width, rows = image_ref.shape
    size = rows // chunks
    steps = 2 * chunks
    me = lax.axis_index("dp")
    part = lax.axis_index("mp")
    parity = lax.rem(me, 2)
    near = me + 1 - 2 * parity
    late = 1 - parity
    row = lax.rem(me // 2, 2)
    relayed = parity != row
    direct = jnp.logical_not(relayed)
    members = 2 * parts
    end, final = chunks - 1, steps - 1
    lead = max(3 * width // 4 // 16, 1) * 16

    def cut_rows(cut):
        return pl.ds(lead, width - lead) if cut else pl.ds(0, lead)

    beside = lax.rem(part + 1, parts)
    member = parity * parts + part

    def shifted(by):
        return lax.rem(me + blocks + by, blocks)

    def load(ref, side, index):
        return pltpu.make_async_copy(
            ref.at[:, pl.ds(index * size, size)], raw.at[0, side, 0, index], load_sem)

    for index in range(chunks):
        load(image_ref, IMAGE, index).start()
        load(text_ref, TEXT, index).start()
    constants[member] = constant_ref[...]

    def settle(ref, sem):
        pltpu.make_async_copy(ref, ref, sem).wait()

    def mate(offset):
        other = lax.rem(member + offset, members)
        return {"dp": me - parity + other // parts, "mp": lax.rem(other, parts)}

    def constant_copy(offset):
        return pltpu.make_async_remote_copy(
            src_ref=constant_ref, dst_ref=constants.at[member],
            send_sem=constant_send, recv_sem=constant_recv,
            device_id=mate(offset), device_id_type=MESH)

    def side_of(step):
        return jnp.where(step < chunks, parity, 1 - parity)

    def piece(k, side, slot, step):
        return raw.at[k, side, slot, lax.rem(step, chunks)]

    def far_copy(step):
        side = side_of(step)
        return pltpu.make_async_remote_copy(
            src_ref=piece(0, side, 0, step), dst_ref=piece(2, side, 0, step),
            send_sem=far_send, recv_sem=far_recv.at[step],
            device_id={"dp": shifted(4 * side - 2)}, device_id_type=MESH)

    def leg_copy(index):
        return pltpu.make_async_remote_copy(
            src_ref=raw.at[0, late, 0, index], dst_ref=relay.at[index],
            send_sem=leg_send, recv_sem=leg_recv.at[index],
            device_id={"dp": shifted(8 * late - 4)}, device_id_type=MESH)

    def relay_copy(index):
        return pltpu.make_async_remote_copy(
            src_ref=relay.at[index], dst_ref=raw.at[2, late, 0, index],
            send_sem=far_send, recv_sem=far_recv.at[chunks + index],
            device_id={"dp": shifted(2 - 4 * late)}, device_id_type=MESH)

    def near_copy(step, k):
        side = 1 - side_of(step)
        return pltpu.make_async_remote_copy(
            src_ref=piece(k, side, 0, step), dst_ref=piece(1, side, 0, step),
            send_sem=near_send, recv_sem=near_recv.at[step],
            device_id={"dp": near}, device_id_type=MESH)

    def end_piece(k, side, slot, cut):
        return raw.at[k, side, slot, end, cut_rows(cut)]

    def far_end(cut):
        return pltpu.make_async_remote_copy(
            src_ref=end_piece(0, late, 0, cut), dst_ref=end_piece(2, late, parts - 1, cut),
            send_sem=far_send, recv_sem=far_recv.at[final + cut],
            device_id={"dp": shifted(4 * late - 2), "mp": beside}, device_id_type=MESH)

    def relay_end(cut):
        return pltpu.make_async_remote_copy(
            src_ref=relay.at[end, cut_rows(cut)], dst_ref=end_piece(2, late, parts - 1, cut),
            send_sem=far_send, recv_sem=far_recv.at[final + cut],
            device_id={"dp": shifted(2 - 4 * late), "mp": beside}, device_id_type=MESH)

    def near_end(cut):
        return pltpu.make_async_remote_copy(
            src_ref=end_piece(2, parity, 0, cut), dst_ref=end_piece(1, parity, parts - 1, cut),
            send_sem=near_send, recv_sem=near_recv.at[final + cut],
            device_id={"dp": near, "mp": beside}, device_id_type=MESH)

    def share_end(k, cut, offset):
        return pltpu.make_async_remote_copy(
            src_ref=end_piece(k, late, parts - 1, cut), dst_ref=end_piece(k, late, parts - 1 - offset, cut),
            send_sem=share_send.at[offset - 1], recv_sem=share_recv.at[final, parts - offset - 1],
            device_id={"mp": lax.rem(part + offset, parts)}, device_id_type=MESH)

    def own_copy(side, offset):
        return pltpu.make_async_remote_copy(
            src_ref=raw.at[0, side, 0], dst_ref=raw.at[0, side, parts - offset],
            send_sem=own_send.at[offset - 1], recv_sem=own_recv.at[parts - offset - 1],
            device_id={"mp": lax.rem(part + offset, parts)}, device_id_type=MESH)

    def share_copy(k, step, offset):
        side = side_of(step)
        return pltpu.make_async_remote_copy(
            src_ref=piece(k, side, 0, step), dst_ref=piece(k, side, parts - offset, step),
            send_sem=share_send.at[offset - 1], recv_sem=share_recv.at[step, parts - offset - 1],
            device_id={"mp": lax.rem(part + offset, parts)}, device_id_type=MESH)

    barrier = pltpu.get_barrier_semaphore()

    def greet(target):
        pl.semaphore_signal(barrier, inc=1, device_id={"dp": target}, device_id_type=MESH)

    greet(shifted(2 - 4 * row))
    pl.semaphore_signal(
        barrier, inc=1, device_id={"dp": shifted(2 - 4 * row), "mp": lax.rem(part + parts - 1, parts)},
        device_id_type=MESH)

    @pl.when(relayed)
    def _():
        greet(shifted(-2 - 2 * row))

    for offset in range(1, members):
        pl.semaphore_signal(barrier, inc=1, device_id=mate(offset), device_id_type=MESH)
    settle(raw.at[0, :, 0], load_sem)
    pl.semaphore_wait(barrier, 1 + row + members)

    for offset in range(1, members):
        constant_copy(offset).start()

    def inform(target):
        pl.semaphore_signal(token, inc=1, device_id={"dp": target}, device_id_type=MESH)

    @pl.when(row == 1)
    def _():
        inform(shifted(4 - 2 * parity))

    for step in range(chunks):
        @pl.when(parity + row > 0)
        def _():
            far_copy(step).start()

        near_copy(step, 0).start()

    @pl.when(direct)
    def _():
        for step in range(chunks, final):
            far_copy(step).start()
        for cut in (0, 1):
            far_end(cut).start()

    for side in (IMAGE, TEXT):
        for offset in range(1, parts):
            own_copy(side, offset).start()

    def unit_rows(k, side, index):
        wide = [raw[k, side, slot, index].astype(F32) for slot in range(parts)]
        square = sum(jnp.sum(w * w, axis=0, keepdims=True) for w in wide)
        inverse = lax.rsqrt(square + 1e-06)
        return [(w * inverse).astype(BF16) for w in wide], inverse

    def pair_terms(units, side, diagonal):
        other = 1 - side
        scale = jnp.exp(constants[0, :, 0:1])
        bias = constants[1, :, 0:1]
        weight = scale * constants[2, :, 0:1]
        total = jnp.dot(own_rows[other], jnp.concatenate(units, axis=0), preferred_element_type=F32)
        scores = scale * total + bias
        if diagonal:
            shape = total.shape
            matching = lax.broadcasted_iota(jnp.int32, shape, 0) == lax.broadcasted_iota(jnp.int32, shape, 1)
            sign = jnp.where(matching, 1.0, -1.0).astype(F32)
            factor = -weight * sign * jax.nn.sigmoid(-sign * scores)
        else:
            factor = weight * jax.nn.sigmoid(scores)
        factor = factor.astype(BF16)
        gradient = lax.dot_general(
            units[0], factor, (((1,), (1,)), ((), ())), preferred_element_type=F32)
        product = factor.astype(F32) * total
        product = sum(product[:, at:at + size] for at in range(0, product.shape[1], size))
        if diagonal:
            sums[other] = gradient
            inner[other] = product
        else:
            sums[other] += gradient
            inner[other] += product

    @pl.when((parity == 0) & (row == 1))
    def _():
        for index in range(chunks):
            leg_copy(index).start()
        pl.semaphore_wait(token, 1)
        inform(shifted(-2))

    @pl.when((parity == 0) & (row == 0))
    def _():
        pl.semaphore_wait(token, 1)
        for step in range(chunks):
            far_copy(step).start()

    @pl.when((parity == 1) & (row == 0))
    def _():
        pl.semaphore_wait(token, 1)
        for index in range(chunks):
            leg_copy(index).start()

    for slot in range(1, parts):
        settle(raw.at[0, :, slot], own_recv.at[slot - 1])

    def own_norm(index, carry):
        side, place = index // chunks, lax.rem(index, chunks)
        units, inverse = unit_rows(0, side, place)
        for slot in range(parts):
            own_unit[side, slot, place] = units[slot]
        own_rows[side, pl.ds(pl.multiple_of(place * size, size), size), :] = jnp.concatenate(units, axis=0).T
        own_inverse[side, place] = inverse
        return carry

    lax.fori_loop(0, steps, own_norm, 0)
    settle(constants.at[pl.ds(1, members - 1)], constant_recv)

    def own_pairs(side, carry):
        pair_terms(
            [jnp.concatenate([own_unit[side, slot, place] for place in range(chunks)], axis=1)
             for slot in range(parts)], side, True)
        return carry

    lax.fori_loop(0, 2, own_pairs, 0)

    def place_of(index):
        return slice(index * size, (index + 1) * size)

    def early_finish():
        for index in range(chunks):
            place = place_of(index)
            early_out[:, place] = finish(
                sums[late, :, place], inner[late, place], own_inverse[late, index],
                raw[0, late, 0, index].astype(F32) * own_inverse[late, index])
            unit_out[:, place] = raw[0, parity, 0, index].astype(F32) * own_inverse[parity, index]

    def band_pairs(step):
        side = side_of(step)
        for slot in range(1, parts):
            settle(raw.at[pl.ds(1, 2), side, slot, lax.rem(step, chunks)], share_recv.at[step, slot - 1])
        units = [unit_rows(k, side, lax.rem(step, chunks))[0] for k in (1, 2)]
        pair_terms([jnp.concatenate(halves, axis=1) for halves in zip(*units)], side, False)

    def arrive(step):
        far_copy(step).wait_recv()

        @pl.when(step < end)
        def _():
            near_copy(step + chunks, 2).start()

        @pl.when(step == end)
        def _():
            for cut in (0, 1):
                near_end(cut).start()

        @pl.when((step < chunks) & relayed)
        def _():
            leg_copy(step).wait_recv()

            @pl.when(step < end)
            def _():
                relay_copy(step).start()

            @pl.when(step == end)
            def _():
                for cut in (0, 1):
                    relay_end(cut).start()

        for offset in range(1, parts):
            share_copy(2, step, offset).start()
        near_copy(step, 0).wait_recv()
        for offset in range(1, parts):
            share_copy(1, step, offset).start()

    def arrive_end():
        for cut in (0, 1):
            far_end(cut).wait_recv()
            for offset in range(1, parts):
                share_end(2, cut, offset).start()
            near_end(cut).wait_recv()
            for offset in range(1, parts):
                share_end(1, cut, offset).start()

    def advance(step, carry):
        @pl.when(step < final)
        def _():
            arrive(step)

        @pl.when(step == final)
        def _():
            arrive_end()

        @pl.when(step > 0)
        def _():
            band_pairs(step - 1)

        @pl.when(step == chunks)
        def _():
            early_finish()

        return carry

    lax.fori_loop(0, steps + 1, advance, 0)

    @pl.when(relayed)
    def _():
        settle(relay, leg_send)

    settle(raw.at[0, :, 0], far_send)
    settle(raw.at[0, :, 0], near_send)
    settle(constants.at[pl.ds(1, members - 1)], constant_send)
    for offset in range(1, parts):
        settle(raw.at[0, :, 0], own_send.at[offset - 1])
        settle(raw.at[pl.ds(0, 2), :, 0], share_send.at[offset - 1])


def spread(value_ref, row_ref):
    row_ref[...] = jnp.full(row_ref.shape, value_ref[0])


def finish(gradient, products, inverse, unit):
    inner = jnp.sum(products.T, axis=0, keepdims=True)
    return inverse * (gradient - unit * inner)


def publish(early_ref, unit_ref, sums, inner, own_inverse, image_out, text_out, late_ref, early_sem, late_sem):
    parity = lax.rem(lax.axis_index("dp"), 2)
    chunks, _, size = own_inverse.shape[1:]

    def emit(first, second, ref, place, sem):
        @pl.when(parity == 0)
        def _():
            pltpu.make_async_copy(ref.at[:, place], first.at[:, place], sem).start()

        @pl.when(parity == 1)
        def _():
            pltpu.make_async_copy(ref.at[:, place], second.at[:, place], sem).start()

    emit(text_out, image_out, early_ref, slice(None), early_sem)
    for index in range(chunks):
        place = slice(index * size, (index + 1) * size)
        late_ref[:, place] = finish(
            sums[parity, :, place], inner[parity, place], own_inverse[parity, index], unit_ref[:, place])
        emit(image_out, text_out, late_ref, place, late_sem)
    pltpu.make_async_copy(early_ref, early_ref, early_sem).wait()
    pltpu.make_async_copy(late_ref, late_ref, late_sem).wait()


def solution(mesh):
    blocks, parts = mesh.shape["dp"], mesh.shape["mp"]

    def local(image, text, log_logit_scale, bias, loss_upstream_gradient):
        rows, width = image.shape
        chunks = max(rows // 128, 1)
        size = rows // chunks
        steps = 2 * chunks
        hbm = pl.BlockSpec(memory_space=pltpu.HBM)
        whole = pl.BlockSpec(memory_space=pltpu.VMEM)
        dma = pltpu.SemaphoreType.DMA
        out = jax.ShapeDtypeStruct((width, rows), F32)
        member = lax.rem(lax.axis_index("dp"), 2) * parts + lax.axis_index("mp")

        def pick(place):
            def branch(*values):
                return pl.pallas_call(
                    spread,
                    out_shape=pltpu.VMEM((1, 128), F32),
                    in_specs=[pl.BlockSpec(memory_space=pltpu.SMEM)],
                    out_specs=whole,
                    name=f"constant_{place}",
                    compiler_params=pltpu.CompilerParams(vmem_limit_bytes=1 << 20),
                )(values[place].reshape(1))
            return branch

        constant = lax.switch(
            lax.rem(member, 3), [pick(place) for place in range(3)], log_logit_scale, bias, loss_upstream_gradient)
        results = pl.pallas_call(
            functools.partial(kernel, blocks, parts, chunks),
            out_shape=(
                pltpu.VMEM((width, rows), F32), pltpu.VMEM((width, rows), F32),
                pltpu.VMEM((2, width, rows), F32), pltpu.VMEM((2, rows, size), F32),
                pltpu.VMEM((2, chunks, 1, size), F32)),
            in_specs=[hbm, hbm, whole],
            out_specs=(whole,) * 5,
            scratch_shapes=[
                pltpu.VMEM((3, 2, parts, chunks, width, size), BF16),
                pltpu.VMEM((chunks, width, size), BF16),
                pltpu.VMEM((2, parts, chunks, width, size), BF16),
                pltpu.VMEM((2, rows, parts * width), BF16),
                pltpu.VMEM((2 * parts, 1, 128), F32),
                dma, dma, dma, dma, dma((steps + 1,)), dma, dma((steps + 1,)), dma, dma((chunks,)),
                dma((parts - 1,)), dma((parts - 1,)),
                dma((parts - 1,)), dma((steps, parts - 1)), pltpu.SemaphoreType.REGULAR,
            ],
            compiler_params=pltpu.CompilerParams(
                collective_id=0, has_side_effects=True, vmem_limit_bytes=VMEM_LIMIT),
        )(image.T, text.T, constant)
        image_grad, text_grad = pl.pallas_call(
            publish,
            out_shape=(out, out),
            in_specs=[whole] * 5,
            out_specs=(hbm, hbm),
            scratch_shapes=[pltpu.VMEM((width, rows), F32), dma, dma],
            compiler_params=pltpu.CompilerParams(vmem_limit_bytes=16 << 20),
        )(*results)
        return image_grad.T, text_grad.T

    placed = (P("dp", "mp"), P("dp", "mp"), P(), P(), P())
    return jax.shard_map(
        local, mesh=mesh, in_specs=placed, out_specs=(P("dp", "mp"), P("dp", "mp")), check_vma=False
    )
```

```python
import functools

import jax
import jax.numpy as jnp
from jax import lax
from jax.experimental import pallas as pl
from jax.experimental.pallas import tpu as pltpu
from jax.sharding import PartitionSpec as P

MESH = pl.DeviceIdType.MESH
F32 = jnp.float32
BF16 = jnp.bfloat16
IMAGE, TEXT = 0, 1
VMEM_LIMIT = 60 << 20


def kernel(
    blocks, parts, chunks,
    image_ref, text_ref, constant_ref,
    early_out, unit_out, sums, inner, own_inverse,
    raw, relay, own_unit, own_rows, constants,
    load_sem, constant_send, constant_recv, far_send, far_recv, near_send, near_recv, leg_send, leg_recv,
    own_send, own_recv, share_send, share_recv, token,
):
    width, rows = image_ref.shape
    size = rows // chunks
    steps = 2 * chunks
    me = lax.axis_index("dp")
    part = lax.axis_index("mp")
    parity = lax.rem(me, 2)
    near = me + 1 - 2 * parity
    late = 1 - parity
    row = lax.rem(me // 2, 2)
    relayed = parity != row
    direct = jnp.logical_not(relayed)
    members = 2 * parts
    end, final = chunks - 1, steps - 1
    lead = max(3 * width // 4 // 16, 1) * 16

    def cut_rows(cut):
        return pl.ds(lead, width - lead) if cut else pl.ds(0, lead)

    beside = lax.rem(part + 1, parts)
    member = parity * parts + part

    def shifted(by):
        return lax.rem(me + blocks + by, blocks)

    def load(ref, side, index):
        return pltpu.make_async_copy(
            ref.at[:, pl.ds(index * size, size)], raw.at[0, side, 0, index], load_sem)

    for index in range(chunks):
        load(image_ref, IMAGE, index).start()
        load(text_ref, TEXT, index).start()
    constants[member] = constant_ref[...]

    def settle(ref, sem):
        pltpu.make_async_copy(ref, ref, sem).wait()

    def mate(offset):
        other = lax.rem(member + offset, members)
        return {"dp": me - parity + other // parts, "mp": lax.rem(other, parts)}

    def constant_copy(offset):
        return pltpu.make_async_remote_copy(
            src_ref=constant_ref, dst_ref=constants.at[member],
            send_sem=constant_send, recv_sem=constant_recv,
            device_id=mate(offset), device_id_type=MESH)

    def side_of(step):
        return jnp.where(step < chunks, parity, 1 - parity)

    def piece(k, side, slot, step):
        return raw.at[k, side, slot, lax.rem(step, chunks)]

    def far_copy(step):
        side = side_of(step)
        return pltpu.make_async_remote_copy(
            src_ref=piece(0, side, 0, step), dst_ref=piece(2, side, 0, step),
            send_sem=far_send, recv_sem=far_recv.at[step],
            device_id={"dp": shifted(4 * side - 2)}, device_id_type=MESH)

    def leg_copy(index):
        return pltpu.make_async_remote_copy(
            src_ref=raw.at[0, late, 0, index], dst_ref=relay.at[index],
            send_sem=leg_send, recv_sem=leg_recv.at[index],
            device_id={"dp": shifted(8 * late - 4)}, device_id_type=MESH)

    def relay_copy(index):
        return pltpu.make_async_remote_copy(
            src_ref=relay.at[index], dst_ref=raw.at[2, late, 0, index],
            send_sem=far_send, recv_sem=far_recv.at[chunks + index],
            device_id={"dp": shifted(2 - 4 * late)}, device_id_type=MESH)

    def near_copy(step, k):
        side = 1 - side_of(step)
        return pltpu.make_async_remote_copy(
            src_ref=piece(k, side, 0, step), dst_ref=piece(1, side, 0, step),
            send_sem=near_send, recv_sem=near_recv.at[step],
            device_id={"dp": near}, device_id_type=MESH)

    def end_piece(k, side, slot, cut):
        return raw.at[k, side, slot, end, cut_rows(cut)]

    def far_end(cut):
        return pltpu.make_async_remote_copy(
            src_ref=end_piece(0, late, 0, cut), dst_ref=end_piece(2, late, parts - 1, cut),
            send_sem=far_send, recv_sem=far_recv.at[final + cut],
            device_id={"dp": shifted(4 * late - 2), "mp": beside}, device_id_type=MESH)

    def relay_end(cut):
        return pltpu.make_async_remote_copy(
            src_ref=relay.at[end, cut_rows(cut)], dst_ref=end_piece(2, late, parts - 1, cut),
            send_sem=far_send, recv_sem=far_recv.at[final + cut],
            device_id={"dp": shifted(2 - 4 * late), "mp": beside}, device_id_type=MESH)

    def near_end(cut):
        return pltpu.make_async_remote_copy(
            src_ref=end_piece(2, parity, 0, cut), dst_ref=end_piece(1, parity, parts - 1, cut),
            send_sem=near_send, recv_sem=near_recv.at[final + cut],
            device_id={"dp": near, "mp": beside}, device_id_type=MESH)

    def share_end(k, cut, offset):
        return pltpu.make_async_remote_copy(
            src_ref=end_piece(k, late, parts - 1, cut), dst_ref=end_piece(k, late, parts - 1 - offset, cut),
            send_sem=share_send.at[offset - 1], recv_sem=share_recv.at[final, parts - offset - 1],
            device_id={"mp": lax.rem(part + offset, parts)}, device_id_type=MESH)

    def own_copy(side, offset):
        return pltpu.make_async_remote_copy(
            src_ref=raw.at[0, side, 0], dst_ref=raw.at[0, side, parts - offset],
            send_sem=own_send.at[offset - 1], recv_sem=own_recv.at[parts - offset - 1],
            device_id={"mp": lax.rem(part + offset, parts)}, device_id_type=MESH)

    def share_copy(k, step, offset):
        side = side_of(step)
        return pltpu.make_async_remote_copy(
            src_ref=piece(k, side, 0, step), dst_ref=piece(k, side, parts - offset, step),
            send_sem=share_send.at[offset - 1], recv_sem=share_recv.at[step, parts - offset - 1],
            device_id={"mp": lax.rem(part + offset, parts)}, device_id_type=MESH)

    barrier = pltpu.get_barrier_semaphore()

    def greet(target):
        pl.semaphore_signal(barrier, inc=1, device_id={"dp": target}, device_id_type=MESH)

    greet(shifted(2 - 4 * row))
    pl.semaphore_signal(
        barrier, inc=1, device_id={"dp": shifted(2 - 4 * row), "mp": lax.rem(part + parts - 1, parts)},
        device_id_type=MESH)

    @pl.when(relayed)
    def _():
        greet(shifted(-2 - 2 * row))

    for offset in range(1, members):
        pl.semaphore_signal(barrier, inc=1, device_id=mate(offset), device_id_type=MESH)
    settle(raw.at[0, :, 0], load_sem)
    pl.semaphore_wait(barrier, 1 + row + members)

    for offset in range(1, members):
        constant_copy(offset).start()

    def inform(target):
        pl.semaphore_signal(token, inc=1, device_id={"dp": target}, device_id_type=MESH)

    @pl.when(row == 1)
    def _():
        inform(shifted(4 - 2 * parity))

    for step in range(chunks):
        @pl.when(parity + row > 0)
        def _():
            far_copy(step).start()

        near_copy(step, 0).start()

    @pl.when(direct)
    def _():
        for step in range(chunks, final):
            far_copy(step).start()
        for cut in (0, 1):
            far_end(cut).start()

    for side in (IMAGE, TEXT):
        for offset in range(1, parts):
            own_copy(side, offset).start()

    def unit_rows(k, side, index):
        wide = [raw[k, side, slot, index].astype(F32) for slot in range(parts)]
        square = sum(jnp.sum(w * w, axis=0, keepdims=True) for w in wide)
        inverse = lax.rsqrt(square + 1e-06)
        return [(w * inverse).astype(BF16) for w in wide], inverse

    def pair_terms(units, side, diagonal):
        other = 1 - side
        scale = jnp.exp(constants[0, :, 0:1])
        bias = constants[1, :, 0:1]
        weight = scale * constants[2, :, 0:1]
        total = jnp.dot(own_rows[other], jnp.concatenate(units, axis=0), preferred_element_type=F32)
        scores = scale * total + bias
        if diagonal:
            shape = total.shape
            matching = lax.broadcasted_iota(jnp.int32, shape, 0) == lax.broadcasted_iota(jnp.int32, shape, 1)
            sign = jnp.where(matching, 1.0, -1.0).astype(F32)
            factor = -weight * sign * jax.nn.sigmoid(-sign * scores)
        else:
            factor = weight * jax.nn.sigmoid(scores)
        factor = factor.astype(BF16)
        gradient = lax.dot_general(
            units[0], factor, (((1,), (1,)), ((), ())), preferred_element_type=F32)
        product = factor.astype(F32) * total
        product = sum(product[:, at:at + size] for at in range(0, product.shape[1], size))
        if diagonal:
            sums[other] = gradient
            inner[other] = product
        else:
            sums[other] += gradient
            inner[other] += product

    @pl.when((parity == 0) & (row == 1))
    def _():
        for index in range(chunks):
            leg_copy(index).start()
        pl.semaphore_wait(token, 1)
        inform(shifted(-2))

    @pl.when((parity == 0) & (row == 0))
    def _():
        pl.semaphore_wait(token, 1)
        for step in range(chunks):
            far_copy(step).start()

    @pl.when((parity == 1) & (row == 0))
    def _():
        pl.semaphore_wait(token, 1)
        for index in range(chunks):
            leg_copy(index).start()

    for slot in range(1, parts):
        settle(raw.at[0, :, slot], own_recv.at[slot - 1])

    def own_norm(index, carry):
        side, place = index // chunks, lax.rem(index, chunks)
        units, inverse = unit_rows(0, side, place)
        for slot in range(parts):
            own_unit[side, slot, place] = units[slot]
        own_rows[side, pl.ds(pl.multiple_of(place * size, size), size), :] = jnp.concatenate(units, axis=0).T
        own_inverse[side, place] = inverse
        return carry

    lax.fori_loop(0, steps, own_norm, 0)
    settle(constants.at[pl.ds(1, members - 1)], constant_recv)

    def own_pairs(side, carry):
        pair_terms(
            [jnp.concatenate([own_unit[side, slot, place] for place in range(chunks)], axis=1)
             for slot in range(parts)], side, True)
        return carry

    lax.fori_loop(0, 2, own_pairs, 0)

    def place_of(index):
        return slice(index * size, (index + 1) * size)

    def early_finish():
        for index in range(chunks):
            place = place_of(index)
            early_out[:, place] = finish(
                sums[late, :, place], inner[late, place], own_inverse[late, index],
                raw[0, late, 0, index].astype(F32) * own_inverse[late, index])
            unit_out[:, place] = raw[0, parity, 0, index].astype(F32) * own_inverse[parity, index]

    def band_pairs(step):
        side = side_of(step)
        for slot in range(1, parts):
            settle(raw.at[pl.ds(1, 2), side, slot, lax.rem(step, chunks)], share_recv.at[step, slot - 1])
        units = [unit_rows(k, side, lax.rem(step, chunks))[0] for k in (1, 2)]
        pair_terms([jnp.concatenate(halves, axis=1) for halves in zip(*units)], side, False)

    def arrive(step):
        far_copy(step).wait_recv()

        @pl.when(step < end)
        def _():
            near_copy(step + chunks, 2).start()

        @pl.when(step == end)
        def _():
            for cut in (0, 1):
                near_end(cut).start()

        @pl.when((step < chunks) & relayed)
        def _():
            leg_copy(step).wait_recv()

            @pl.when(step < end)
            def _():
                relay_copy(step).start()

            @pl.when(step == end)
            def _():
                for cut in (0, 1):
                    relay_end(cut).start()

        for offset in range(1, parts):
            share_copy(2, step, offset).start()
        near_copy(step, 0).wait_recv()
        for offset in range(1, parts):
            share_copy(1, step, offset).start()

    def arrive_end():
        for cut in (0, 1):
            near_end(cut).wait_recv()
            for offset in range(1, parts):
                share_end(1, cut, offset).start()
            far_end(cut).wait_recv()
            for offset in range(1, parts):
                share_end(2, cut, offset).start()

    def advance(step, carry):
        @pl.when(step < final)
        def _():
            arrive(step)

        @pl.when(step == final)
        def _():
            arrive_end()

        @pl.when(step > 0)
        def _():
            band_pairs(step - 1)

        @pl.when(step == chunks)
        def _():
            early_finish()

        return carry

    lax.fori_loop(0, steps + 1, advance, 0)

    @pl.when(relayed)
    def _():
        settle(relay, leg_send)

    settle(raw.at[0, :, 0], far_send)
    settle(raw.at[0, :, 0], near_send)
    settle(constants.at[pl.ds(1, members - 1)], constant_send)
    for offset in range(1, parts):
        settle(raw.at[0, :, 0], own_send.at[offset - 1])
        settle(raw.at[pl.ds(0, 2), :, 0], share_send.at[offset - 1])


def spread(value_ref, row_ref):
    row_ref[...] = jnp.full(row_ref.shape, value_ref[0])


def finish(gradient, products, inverse, unit):
    inner = jnp.sum(products.T, axis=0, keepdims=True)
    return inverse * (gradient - unit * inner)


def publish(early_ref, unit_ref, sums, inner, own_inverse, image_out, text_out, late_ref, early_sem, late_sem):
    parity = lax.rem(lax.axis_index("dp"), 2)
    chunks, _, size = own_inverse.shape[1:]

    def emit(first, second, ref, place, sem):
        @pl.when(parity == 0)
        def _():
            pltpu.make_async_copy(ref.at[:, place], first.at[:, place], sem).start()

        @pl.when(parity == 1)
        def _():
            pltpu.make_async_copy(ref.at[:, place], second.at[:, place], sem).start()

    emit(text_out, image_out, early_ref, slice(None), early_sem)
    for index in range(chunks):
        place = slice(index * size, (index + 1) * size)
        late_ref[:, place] = finish(
            sums[parity, :, place], inner[parity, place], own_inverse[parity, index], unit_ref[:, place])
        emit(image_out, text_out, late_ref, place, late_sem)
    pltpu.make_async_copy(early_ref, early_ref, early_sem).wait()
    pltpu.make_async_copy(late_ref, late_ref, late_sem).wait()


def solution(mesh):
    blocks, parts = mesh.shape["dp"], mesh.shape["mp"]

    def local(image, text, log_logit_scale, bias, loss_upstream_gradient):
        rows, width = image.shape
        chunks = max(rows // 128, 1)
        size = rows // chunks
        steps = 2 * chunks
        hbm = pl.BlockSpec(memory_space=pltpu.HBM)
        whole = pl.BlockSpec(memory_space=pltpu.VMEM)
        dma = pltpu.SemaphoreType.DMA
        out = jax.ShapeDtypeStruct((width, rows), F32)
        member = lax.rem(lax.axis_index("dp"), 2) * parts + lax.axis_index("mp")

        def pick(place):
            def branch(*values):
                return pl.pallas_call(
                    spread,
                    out_shape=pltpu.VMEM((1, 128), F32),
                    in_specs=[pl.BlockSpec(memory_space=pltpu.SMEM)],
                    out_specs=whole,
                    name=f"constant_{place}",
                    compiler_params=pltpu.CompilerParams(vmem_limit_bytes=1 << 20),
                )(values[place].reshape(1))
            return branch

        constant = lax.switch(
            lax.rem(member, 3), [pick(place) for place in range(3)], log_logit_scale, bias, loss_upstream_gradient)
        results = pl.pallas_call(
            functools.partial(kernel, blocks, parts, chunks),
            out_shape=(
                pltpu.VMEM((width, rows), F32), pltpu.VMEM((width, rows), F32),
                pltpu.VMEM((2, width, rows), F32), pltpu.VMEM((2, rows, size), F32),
                pltpu.VMEM((2, chunks, 1, size), F32)),
            in_specs=[hbm, hbm, whole],
            out_specs=(whole,) * 5,
            scratch_shapes=[
                pltpu.VMEM((3, 2, parts, chunks, width, size), BF16),
                pltpu.VMEM((chunks, width, size), BF16),
                pltpu.VMEM((2, parts, chunks, width, size), BF16),
                pltpu.VMEM((2, rows, parts * width), BF16),
                pltpu.VMEM((2 * parts, 1, 128), F32),
                dma, dma, dma, dma, dma((steps + 1,)), dma, dma((steps + 1,)), dma, dma((chunks,)),
                dma((parts - 1,)), dma((parts - 1,)),
                dma((parts - 1,)), dma((steps, parts - 1)), pltpu.SemaphoreType.REGULAR,
            ],
            compiler_params=pltpu.CompilerParams(
                collective_id=0, has_side_effects=True, vmem_limit_bytes=VMEM_LIMIT),
        )(image.T, text.T, constant)
        image_grad, text_grad = pl.pallas_call(
            publish,
            out_shape=(out, out),
            in_specs=[whole] * 5,
            out_specs=(hbm, hbm),
            scratch_shapes=[pltpu.VMEM((width, rows), F32), dma, dma],
            compiler_params=pltpu.CompilerParams(vmem_limit_bytes=16 << 20),
        )(*results)
        return image_grad.T, text_grad.T

    placed = (P("dp", "mp"), P("dp", "mp"), P(), P(), P())
    return jax.shard_map(
        local, mesh=mesh, in_specs=placed, out_specs=(P("dp", "mp"), P("dp", "mp")), check_vma=False
    )
```
